512 devices in a mesh: narrow: 8 (over z), wide: 64 (over x, y, core).
Axes of the slice: x: 4, y: 8, z: 8, core: 2. Of those that a mesh axis runs over, the one named last changes fastest.
Arguments:
- momentum: float32 [4096, 28672], P('narrow', 'wide'), may hold values from -16 to 16
- gradient: bfloat16 [4096, 28672], P('narrow', 'wide'), may hold values from -6 to 6
- right_basis: float32 [28672, 256], P('wide'), may hold values from -0.03125 to 0.03125
- signs: int32 [4096], replicated, may hold values from -1 to 1, as said below
- select: int32 [384], replicated, may hold values from 0 to 4095, as said below
Outputs:
- momentum_out: float32 [4096, 28672], P('narrow', 'wide')
- basis_out: float32 [28672, 256], P('wide')
- update: bfloat16 [4096, 28672], P('narrow', 'wide')
The draws below stay inside these ranges and needn't reach their ends.
Inputs may be any that keep to these rules, and one draw needn't show every extreme that they name: `signs`: each entry is -1 or 1. `select`: 384 distinct row numbers.
All inputs are finite; a program needn't handle non-finite values.
Results may differ from the reference program's by a relative error of at most 0.001.
Values sent between devices are 32-bit elements; how exact they have to be, the bound alone decides.
A program may use at most 64 MiB of HBM per device.

```python
import math
import jax
import jax.numpy as jnp
from jax import lax

ROWS = 4096
COLS = 28672
RANK = 256
SKETCH = 384


def draw_signs(key, part):
    return 2 * jax.random.randint(jax.random.fold_in(key, 11), (ROWS,), 0, 2, dtype=jnp.int32) - 1


def draw_select(key, part):
    return jax.random.permutation(jax.random.fold_in(key, 23), ROWS)[:SKETCH].astype(jnp.int32)


def strengthened(drawn, stream_key, source, target, blocks, factor):
    def block_of(dim):
        return (jnp.arange(drawn.shape[dim]) // (drawn.shape[dim] // blocks)).reshape((-1,) + (1,) * (drawn.ndim - 1 - dim))

    near = jax.random.permutation(stream_key, blocks)[block_of(target)]
    second = (block_of(target) + blocks // 2) % blocks
    return jnp.where((block_of(source) == near) | (block_of(source) == second), factor * drawn, drawn)


def block_scale(stream_key, extent, shards, least, high):
    def one(dim, blocks):
        steps = jax.random.uniform(jax.random.fold_in(jax.random.fold_in(stream_key, 6), dim), (blocks,), jnp.float32, least / len(shards), high / len(shards))
        return jnp.repeat(jnp.exp(steps), extent[dim] // blocks).reshape((-1,) + (1,) * (len(extent) - dim - 1))

    loudness = one(*shards[0])
    for cut in shards[1:]:
        loudness = loudness * one(*cut)
    return loudness


def centred(own_key, dims, spread, limit, pieces=(), held_as=jnp.bfloat16):
    values = spread * jax.random.normal(own_key, dims, jnp.float32)
    if pieces:
        values = values * block_scale(own_key, dims, pieces, -0.22, 0.18)
    return jnp.clip(values, -limit, limit).astype(held_as)


def bell_draw_with(rng, shape, deviation, reach, pieces, heavy, held_as=jnp.bfloat16):
    values = deviation * jax.random.normal(rng, shape, jnp.float32)
    if pieces:
        values = values * block_scale(rng, shape, pieces, -0.22, 0.18)
    return jnp.clip(strengthened(values, jax.random.fold_in(rng, 3), *heavy), -reach, reach).astype(held_as)


def setup_inputs(seed: int = 0) -> dict:
    splits = jax.random.split(jax.random.key(seed), 6)
    return {
        "momentum": bell_draw_with(splits[0], (ROWS, COLS), 1.0, 16.0, ((0, 8), (1, 64)), (1, 0, 64, 4.0), jnp.float32),
        "gradient": centred(splits[1], (ROWS, COLS), 1.0, 6.0, ((0, 8), (1, 64))),
        "right_basis": centred(splits[2], (COLS, RANK), COLS ** -0.5, 0.03125, ((0, 64),), jnp.float32),
        "signs": draw_signs(jax.random.fold_in(splits[5], 71), 0),
        "select": draw_select(jax.random.fold_in(splits[5], 71), 0),
    }


decay_mu = 0.95
norm_epsilon = 1e-06

def hadamard_rows(select, sign_part, first_row, row_count):
    columns = first_row + jnp.arange(row_count, dtype=jnp.int32)
    shared_bits = jnp.bitwise_and(select[:, None], columns[None, :])
    parity = jnp.zeros(shared_bits.shape, jnp.int32)
    for bit_index in range(ROWS.bit_length()):
        parity = jnp.bitwise_xor(parity, jnp.bitwise_and(jnp.right_shift(shared_bits, bit_index), 1))
    entries = (1 - 2 * parity).astype(jnp.float32) * sign_part.astype(jnp.float32)[None, :]
    return entries / math.sqrt(SKETCH)

def reference(momentum, gradient, right_basis, signs, select):
    high = lax.Precision.HIGHEST
    summed = momentum + gradient.astype(jnp.float32)
    hadamard = hadamard_rows(select, signs, 0, ROWS)
    left_raw = jnp.dot(summed.astype(jnp.float32), right_basis.astype(jnp.float32), precision=high, preferred_element_type=jnp.float32)
    sketch = jnp.dot(hadamard.astype(jnp.float32), left_raw.astype(jnp.float32), precision=high, preferred_element_type=jnp.float32)
    gram = jnp.dot(sketch.T.astype(jnp.float32), sketch.astype(jnp.float32), precision=high, preferred_element_type=jnp.float32)
    lower_factor = jnp.linalg.cholesky(gram)
    left_basis = jax.scipy.linalg.solve_triangular(lower_factor, left_raw.T, lower=True).T
    right_raw = jnp.dot(summed.T.astype(jnp.float32), left_basis.astype(jnp.float32), precision=high, preferred_element_type=jnp.float32)
    norms = jnp.sqrt(lax.optimization_barrier(jnp.sum(right_raw * right_raw, axis=0)) + norm_epsilon)
    basis_out = right_raw / norms[None, :]
    momentum_out = summed - (1.0 - decay_mu) * jnp.dot(left_basis.astype(jnp.float32), right_raw.T.astype(jnp.float32), precision=high, preferred_element_type=jnp.float32)
    scale_factor = math.sqrt(ROWS * COLS / RANK)
    update = (scale_factor * jnp.dot(left_basis.astype(jnp.float32), basis_out.T.astype(jnp.float32), precision=high, preferred_element_type=jnp.float32)).astype(jnp.bfloat16)
    return (momentum_out, basis_out, update)
```

```python
import functools
import math

import jax
import jax.numpy as jnp
from jax import lax
from jax.experimental import pallas as pl
from jax.experimental.pallas import tpu as pltpu
from jax.sharding import Mesh
from jax.sharding import PartitionSpec as P

ROWS = 4096
COLS = 28672
RANK = 256
SKETCH = 384
Z, X, Y, CORE = "narrow", "wide_0", "wide_1", "wide_2"
WIDE = (X, Y, CORE)
HIGH = lax.Precision.HIGHEST
MESH = pl.DeviceIdType.MESH
BLOCK = 32

decay_mu = 0.95
norm_epsilon = 1e-06


def matmul(a, b):
    return jnp.dot(a, b, precision=HIGH, preferred_element_type=jnp.float32)


def matmul_nt(a, b):
    return lax.dot_general(
        a, b, (((1,), (1,)), ((), ())), precision=HIGH, preferred_element_type=jnp.float32
    )


def matmul_tn(a, b):
    return lax.dot_general(
        a, b, (((0,), (0,)), ((), ())), precision=HIGH, preferred_element_type=jnp.float32
    )


def factor_block(a_ref, inverse_ref, b):
    n = a_ref.shape[0]
    lo, hi = b * BLOCK, (b + 1) * BLOCK
    tile, off = lo // 128, lo % 128
    lane = lax.broadcasted_iota(jnp.int32, (8, 128), 1)
    sub = lax.broadcasted_iota(jnp.int32, (8, 128), 0)
    groups = BLOCK // 8
    rows = [
        a_ref[lo + 8 * q : lo + 8 * q + 8, tile * 128 : (tile + 1) * 128] for q in range(groups)
    ]
    column = {}

    def spread(panel, first):
        for j in range(8 * panel, 8 * panel + 8):
            for q in range(first, groups):
                column[q, j] = jnp.broadcast_to(rows[q][:, off + j : off + j + 1], (8, 128))

    def row_of(value, k):
        return jnp.broadcast_to(value[k : k + 1, :], (8, 128))

    spread(0, 0)
    for p in range(groups):
        if p + 1 < groups:
            spread(p + 1, p)
        for k in range(8):
            kk = 8 * p + k
            here, below = lane == off + kk, sub > k
            root = lax.rsqrt(row_of(column[p, kk], k))
            pivot = jnp.where(here, root, row_of(rows[p], k) * root)
            scaled = {q: column[q, kk] * root for q in range(p, groups)}
            scaled[p] = jnp.where(below, scaled[p], 0.0)
            for j in range(kk + 1, min(8 * (p + 2), BLOCK)):
                share = row_of(column[p, j], k) * root
                for q in range(p, groups):
                    column[q, j] = column[q, j] - scaled[q] * share
            for q in range(p + 1, groups):
                rows[q] = jnp.where(here, 0.0, rows[q]) - scaled[q] * pivot
            rest = jnp.where(here & below, 0.0, rows[p]) - scaled[p] * pivot
            rows[p] = jnp.where(sub == k, pivot, rest)
    corner = jnp.concatenate(
        [
            jnp.where((lane >= off) & (lane <= off + 8 * q + sub), row, 0.0)
            for q, row in enumerate(rows)
        ],
        axis=0,
    )
    solved = matmul(corner, a_ref[tile * 128 : (tile + 1) * 128, :])
    cols = lax.broadcasted_iota(jnp.int32, (BLOCK, n), 1)
    placed = jnp.concatenate(
        [corner if t == tile else jnp.zeros_like(corner) for t in range(n // 128)], axis=1
    )
    solved = jnp.where((cols >= lo) & (cols < hi), placed, solved)
    inverse_ref[lo:hi, :] = jnp.where(cols < hi, solved, 0.0)
    if hi < n:
        start = hi // 128 * 128
        outer = matmul_tn(solved[:, start:], solved)
        cols = lax.broadcasted_iota(jnp.int32, (n - hi, n), 1)
        kept = jnp.where((cols >= lo) & (cols < hi), 0.0, a_ref[hi:n, :])
        a_ref[hi:n, :] = kept - outer[hi - start :, :]


def factors(
    sizes,
    momentum,
    gradient,
    right_basis,
    signs,
    select,
    left_out,
    right_out,
    norm_out,
    summed,
    summed_t,
    part_away,
    part_home,
    core_in,
    chip_sum,
    x_in,
    y_out,
    y_in,
    left_t,
    left_rows,
    parity,
    sketch_out,
    sketch_in,
    sketch_z_out,
    sketch_z,
    sketch_t,
    gram,
    inverse,
    q_out,
    q_in,
    q_all,
    norm_z,
    norm_y,
    norm_x,
    core_sems,
    x_sems,
    y_sems,
    gather_sems,
    sketch_sems,
    q_sems,
    norm_sems,
):
    nz, nx, ny = sizes
    z, x, y, c = (lax.axis_index(name) for name in (Z, X, Y, CORE))
    other = 1 - c
    half = summed.shape[0] // 2
    rank = right_basis.shape[1]

    around = [{CORE: other}]
    around += [{X: lax.rem(x + d, nx)} for d in range(1, nx)]
    around += [{X: lax.rem(x + d, nx), CORE: other} for d in range(1, nx)]
    around += [{Y: lax.rem(y + d, ny)} for d in range(1, ny)]
    around += [{Z: lax.rem(z + d, nz)} for d in range(1, nz)]
    barrier = pltpu.get_barrier_semaphore()
    for device in around:
        pl.semaphore_signal(barrier, inc=1, device_id=device, device_id_type=MESH)

    started = []

    def send(source, target, sems, index, device):
        copy = pltpu.make_async_remote_copy(
            src_ref=source,
            dst_ref=target,
            send_sem=sems.at[0, index],
            recv_sem=sems.at[1, index],
            device_id=device,
            device_id_type=MESH,
        )
        copy.start()
        started.append(copy)
        return copy

    summed[...] = momentum[...] + gradient[...].astype(jnp.float32)
    basis_t = right_basis[...].T
    away = matmul_nt(basis_t, summed[pl.ds(pl.multiple_of(other * half, half), half), :])
    part_away[...] = away.reshape(part_away.shape)
    pl.semaphore_wait(barrier, len(around))
    order = [lax.rem(x + d, nx) for d in range(1, nx)] + [x]
    core_copies = [
        send(part_away.at[to], core_in.at[to], core_sems, i, {CORE: other})
        for i, to in enumerate(order)
    ]
    home = matmul_nt(basis_t, summed[pl.ds(pl.multiple_of(c * half, half), half), :])
    part_home[...] = home.reshape(part_home.shape)

    x_copies = []
    for i, to in enumerate(order):
        core_copies[i].wait_recv()
        total = part_home[to] + core_in[to]
        if i < nx - 1:
            chip_sum[to] = total
            x_copies.append(send(chip_sum.at[to], x_in.at[x], x_sems, i, {X: to}))
        else:
            x_in[x] = total
    place = lax.broadcasted_iota(jnp.int32, parity.shape, 0) + (z * 2 * half + c * half)
    shared = jnp.bitwise_and(place, select[...])
    for shift in (8, 4, 2, 1):
        shared = jnp.bitwise_xor(shared, jnp.right_shift(shared, shift))
    parity[...] = 1.0 - 2.0 * jnp.bitwise_and(shared, 1).astype(jnp.float32)
    for copy in x_copies:
        copy.wait_recv()
    total = x_in[0]
    for i in range(1, nx):
        total = total + x_in[i]
    y_out[...] = total.reshape(y_out.shape)
    y_copies = []
    for d in range(1, ny):
        to = lax.rem(y + d, ny)
        y_copies.append(send(y_out.at[to], y_in.at[y], y_sems, d - 1, {Y: to}))
    y_in[y] = y_out[y]
    summed_t[...] = summed[...].T
    for copy in y_copies:
        copy.wait_recv()
    own = y_in[0]
    for i in range(1, ny):
        own = own + y_in[i]

    mine = x * ny + y

    def along_y(buffer, sems):
        copies = []
        for d in range(1, ny):
            block = buffer.at[c, mine]
            copies.append(send(block, block, sems, d - 1, {Y: lax.rem(y + d, ny)}))
        return copies

    def along_x(buffer, sems, waited):
        for copy in waited:
            copy.wait_recv()
        slab = buffer.at[c, pl.ds(x * ny, ny)]
        copies = []
        for d in range(1, nx):
            copies.append(send(slab, slab, sems, ny - 2 + d, {X: lax.rem(x + d, nx)}))
        return copies, [send(slab, slab, sems, ny + nx - 2, {CORE: other})]

    def along_core(buffer, sems, waited):
        copies = []
        for d, copy in enumerate(waited, 1):
            copy.wait_recv()
            slab = buffer.at[c, pl.ds(lax.rem(x - d + nx, nx) * ny, ny)]
            copies.append(send(slab, slab, sems, ny + nx - 2 + d, {CORE: other}))
        return copies

    left_t[c, mine] = own
    left_y = along_y(left_t, gather_sems.at[0])

    flip = signs[pl.ds(z * 2 + c, 1), :].astype(jnp.float32)
    term = matmul(own * flip, parity[...]) * (1.0 / math.sqrt(SKETCH))
    sketch_out[...] = term
    sketch_copy = send(sketch_out, sketch_in, sketch_sems, 0, {CORE: other})
    sketch_copy.wait_recv()
    term = term + sketch_in[...]
    wide = sketch_z.shape[-1]
    sketch_z_out[0] = term[:, :wide]
    sketch_z_out[1] = term[:, SKETCH - wide :]
    sketch_copies = [
        send(sketch_z_out.at[c], sketch_z.at[z], sketch_sems, d, {Z: lax.rem(z + d, nz)})
        for d in range(1, nz)
    ]
    sketch_z[z] = sketch_z_out[c]

    left_x, left_core = along_x(left_t, gather_sems.at[0], left_y)

    for copy in sketch_copies:
        copy.wait_recv()
    total = sketch_z[0]
    for i in range(1, nz):
        total = total + sketch_z[i]
    sketch_t[c, mine] = total
    sketch_y = along_y(sketch_t, gather_sems.at[1])

    left_core += along_core(left_t, gather_sems.at[0], left_x)
    for copy in left_core:
        copy.wait_recv()

    left_0 = left_t[0].reshape(rank, half)
    left_1 = left_t[1].reshape(rank, half)
    product = matmul_nt(summed_t[:, :half], left_0) + matmul_nt(summed_t[:, half:], left_1)
    q_out[...] = product.reshape(q_out.shape)
    q_copies = []
    for d in range(1, nz):
        to = lax.rem(z + d, nz)
        q_copies.append(send(q_out.at[to], q_in.at[z], q_sems, d - 1, {Z: to}))

    sketch_x, sketch_core = along_x(sketch_t, gather_sems.at[1], sketch_y)
    q_in[z] = q_out[z]
    left_rows[:half, :] = left_0.T
    left_rows[half:, :] = left_1.T
    sketch_core += along_core(sketch_t, gather_sems.at[1], sketch_x)
    for copy in sketch_core:
        copy.wait_recv()

    first = sketch_t[0].reshape(rank, wide)
    last = sketch_t[1].reshape(rank, wide)[:, 2 * wide - SKETCH :]
    gram[...] = matmul_nt(first, first) + matmul_nt(last, last)
    gathered = []
    for b in range(rank // BLOCK):
        factor_block(gram, inverse, b)
        if b == rank // BLOCK // 2:
            for copy in q_copies:
                copy.wait_recv()
            total = q_in[0]
            for i in range(1, nz):
                total = total + q_in[i]
            q_all[z] = total
            for d in range(1, nz):
                block = q_all.at[z]
                to = lax.rem(z + d, nz)
                gathered.append(send(block, block, q_sems, nz - 2 + d, {Z: to}))

    share = matmul_nt(q_all[z], inverse[...])
    norm_z[z] = jnp.sum(share * share, axis=0, keepdims=True)
    copies = [
        send(norm_z.at[z], norm_z.at[z], norm_sems, d, {Z: lax.rem(z + d, nz)})
        for d in range(1, nz)
    ]
    left_out[...] = matmul_nt(left_rows[...], inverse[...])
    for copy in copies:
        copy.wait_recv()
    total = norm_z[0]
    for i in range(1, nz):
        total = total + norm_z[i]
    norm_y[y] = total
    copies = [
        send(norm_y.at[y], norm_y.at[y], norm_sems, nz + d, {Y: lax.rem(y + d, ny)})
        for d in range(1, ny)
    ]
    for copy in copies:
        copy.wait_recv()
    total = norm_y[0]
    for i in range(1, ny):
        total = total + norm_y[i]
    slot = x * 2 + c
    norm_x[slot] = total
    copies = []
    for i, device in enumerate(around[: 2 * nx - 1]):
        copies.append(send(norm_x.at[slot], norm_x.at[slot], norm_sems, nz + ny + i, device))
    for copy in gathered:
        copy.wait_recv()
    right_out[...] = matmul_nt(q_all[...].reshape(right_out.shape), inverse[...])
    for copy in copies:
        copy.wait_recv()
    total = norm_x[0]
    for i in range(1, 2 * nx):
        total = total + norm_x[i]
    norm_out[...] = jnp.sqrt(total + norm_epsilon)
    for copy in started:
        copy.wait_send()


def outputs(
    momentum, gradient, left, right, norms, momentum_out, basis_out, update, basis
):
    @pl.when(pl.program_id(0) == 0)
    def _():
        basis[...] = right[...] / norms[...]
        basis_out[...] = basis[...]

    summed = momentum[...] + gradient[...].astype(jnp.float32)
    momentum_out[...] = summed - (1.0 - decay_mu) * matmul_nt(left[...], right[...])
    update[...] = (math.sqrt(ROWS * COLS / RANK) * matmul_nt(left[...], basis[...])).astype(jnp.bfloat16)


def per_device(sizes, momentum, gradient, right_basis, signs, select):
    nz, nx, ny = sizes
    block_rows, block_cols = momentum.shape
    rank = right_basis.shape[1]
    half = block_rows // 2
    own = rank // (nx * ny)
    wide = 256
    f32 = jnp.float32
    vmem = pl.BlockSpec(memory_space=pltpu.VMEM)
    dma = pltpu.SemaphoreType.DMA
    share = block_cols // nz
    left, right, norms = pl.pallas_call(
        functools.partial(factors, sizes),
        out_shape=(
            jax.ShapeDtypeStruct((block_rows, rank), f32),
            jax.ShapeDtypeStruct((block_cols, rank), f32),
            jax.ShapeDtypeStruct((1, rank), f32),
        ),
        in_specs=[vmem] * 5,
        out_specs=(vmem,) * 3,
        scratch_shapes=[
            pltpu.VMEM((block_rows, block_cols), f32),
            pltpu.VMEM((block_cols, block_rows), f32),
            pltpu.VMEM((nx, rank // nx, half), f32),
            pltpu.VMEM((nx, rank // nx, half), f32),
            pltpu.VMEM((nx, rank // nx, half), f32),
            pltpu.VMEM((nx, rank // nx, half), f32),
            pltpu.VMEM((nx, rank // nx, half), f32),
            pltpu.VMEM((ny, own, half), f32),
            pltpu.VMEM((ny, own, half), f32),
            pltpu.VMEM((2, nx * ny, own, half), f32),
            pltpu.VMEM((block_rows, rank), f32),
            pltpu.VMEM((half, SKETCH), f32),
            pltpu.VMEM((own, SKETCH), f32),
            pltpu.VMEM((own, SKETCH), f32),
            pltpu.VMEM((2, own, wide), f32),
            pltpu.VMEM((nz, own, wide), f32),
            pltpu.VMEM((2, nx * ny, own, wide), f32),
            pltpu.VMEM((rank, rank), f32),
            pltpu.VMEM((rank, rank), f32),
            pltpu.VMEM((nz, share, rank), f32),
            pltpu.VMEM((nz, share, rank), f32),
            pltpu.VMEM((nz, share, rank), f32),
            pltpu.VMEM((nz, 1, rank), f32),
            pltpu.VMEM((ny, 1, rank), f32),
            pltpu.VMEM((2 * nx, 1, rank), f32),
            dma((2, nx)),
            dma((2, nx)),
            dma((2, ny)),
            dma((2, 2, ny + 2 * nx)),
            dma((2, nz)),
            dma((2, 2 * nz)),
            dma((2, nz + ny + 2 * nx)),
        ],
        compiler_params=pltpu.CompilerParams(
            collective_id=0, has_side_effects=True, vmem_limit_bytes=40 << 20
        ),
        name="factors",
    )(
        momentum,
        gradient,
        right_basis,
        signs.reshape(nz * 2, half),
        select.reshape(1, SKETCH),
    )
    rows = min(128, block_rows)
    slab = pl.BlockSpec((rows, block_cols), lambda i: (i, 0))
    whole = pl.BlockSpec((block_cols, rank), lambda i: (0, 0))
    return pl.pallas_call(
        outputs,
        grid=(block_rows // rows,),
        out_shape=(
            jax.ShapeDtypeStruct((block_rows, block_cols), f32),
            jax.ShapeDtypeStruct((block_cols, rank), f32),
            jax.ShapeDtypeStruct((block_rows, block_cols), jnp.bfloat16),
        ),
        in_specs=[
            slab,
            slab,
            pl.BlockSpec((rows, rank), lambda i: (i, 0)),
            whole,
            pl.BlockSpec((1, rank), lambda i: (0, 0)),
        ],
        out_specs=(slab, whole, slab),
        scratch_shapes=[pltpu.VMEM((block_cols, rank), f32)],
        name="outputs",
    )(momentum, gradient, left, right, norms)


def solution(mesh):
    devices = mesh.devices
    shape = (mesh.shape["narrow"], 4, 8, 2) if devices.size == 512 else (2, 2, devices.size // 8, 2)
    split = Mesh(devices.reshape(shape), (Z, X, Y, CORE))
    in_specs = (P(Z, WIDE), P(Z, WIDE), P(WIDE, None), P(), P())
    out_specs = (P(Z, WIDE), P(WIDE, None), P(Z, WIDE))
    return jax.shard_map(
        functools.partial(per_device, shape[:3]),
        mesh=split,
        in_specs=in_specs,
        out_specs=out_specs,
        check_vma=False,
    )
```

```python
import functools
import math

import jax
import jax.numpy as jnp
from jax import lax
from jax.experimental import pallas as pl
from jax.experimental.pallas import tpu as pltpu
from jax.sharding import Mesh
from jax.sharding import PartitionSpec as P

ROWS = 4096
COLS = 28672
RANK = 256
SKETCH = 384
Z, X, Y, CORE = "narrow", "wide_0", "wide_1", "wide_2"
WIDE = (X, Y, CORE)
HIGH = lax.Precision.HIGHEST
MESH = pl.DeviceIdType.MESH
BLOCK = 32

decay_mu = 0.95
norm_epsilon = 1e-06


def matmul(a, b):
    return jnp.dot(a, b, precision=HIGH, preferred_element_type=jnp.float32)


def matmul_nt(a, b):
    return lax.dot_general(
        a, b, (((1,), (1,)), ((), ())), precision=HIGH, preferred_element_type=jnp.float32
    )


def matmul_tn(a, b):
    return lax.dot_general(
        a, b, (((0,), (0,)), ((), ())), precision=HIGH, preferred_element_type=jnp.float32
    )


def factor_block(a_ref, inverse_ref, b):
    n = a_ref.shape[0]
    lo, hi = b * BLOCK, (b + 1) * BLOCK
    tile, off = lo // 128, lo % 128
    lane = lax.broadcasted_iota(jnp.int32, (8, 128), 1)
    sub = lax.broadcasted_iota(jnp.int32, (8, 128), 0)
    groups = BLOCK // 8
    rows = [
        a_ref[lo + 8 * q : lo + 8 * q + 8, tile * 128 : (tile + 1) * 128] for q in range(groups)
    ]
    column = {}

    def spread(panel, first):
        for j in range(8 * panel, 8 * panel + 8):
            for q in range(first, groups):
                column[q, j] = jnp.broadcast_to(rows[q][:, off + j : off + j + 1], (8, 128))

    def row_of(value, k):
        return jnp.broadcast_to(value[k : k + 1, :], (8, 128))

    spread(0, 0)
    for p in range(groups):
        if p + 1 < groups:
            spread(p + 1, p)
        for k in range(8):
            kk = 8 * p + k
            here, below = lane == off + kk, sub > k
            root = lax.rsqrt(row_of(column[p, kk], k))
            pivot = jnp.where(here, root, row_of(rows[p], k) * root)
            scaled = {q: column[q, kk] * root for q in range(p, groups)}
            scaled[p] = jnp.where(below, scaled[p], 0.0)
            for j in range(kk + 1, min(8 * (p + 2), BLOCK)):
                share = row_of(column[p, j], k) * root
                for q in range(p, groups):
                    column[q, j] = column[q, j] - scaled[q] * share
            for q in range(p + 1, groups):
                rows[q] = jnp.where(here, 0.0, rows[q]) - scaled[q] * pivot
            rest = jnp.where(here & below, 0.0, rows[p]) - scaled[p] * pivot
            rows[p] = jnp.where(sub == k, pivot, rest)
    corner = jnp.concatenate(
        [
            jnp.where((lane >= off) & (lane <= off + 8 * q + sub), row, 0.0)
            for q, row in enumerate(rows)
        ],
        axis=0,
    )
    solved = matmul(corner, a_ref[tile * 128 : (tile + 1) * 128, :])
    cols = lax.broadcasted_iota(jnp.int32, (BLOCK, n), 1)
    placed = jnp.concatenate(
        [corner if t == tile else jnp.zeros_like(corner) for t in range(n // 128)], axis=1
    )
    solved = jnp.where((cols >= lo) & (cols < hi), placed, solved)
    inverse_ref[lo:hi, :] = jnp.where(cols < hi, solved, 0.0)
    if hi < n:
        start = hi // 128 * 128
        outer = matmul_tn(solved[:, start:], solved)
        cols = lax.broadcasted_iota(jnp.int32, (n - hi, n), 1)
        kept = jnp.where((cols >= lo) & (cols < hi), 0.0, a_ref[hi:n, :])
        a_ref[hi:n, :] = kept - outer[hi - start :, :]


def factors(
    sizes,
    momentum_in,
    gradient_in,
    basis_in,
    signs_in,
    select_in,
    left_out,
    right_out,
    norm_out,
    summed_out,
    summed_t,
    left,
    right,
    norms,
    momentum,
    gradient,
    right_basis,
    signs,
    select,
    part_away,
    part_home,
    core_in,
    chip_sum,
    x_in,
    y_out,
    y_in,
    left_t,
    parity,
    sketch_out,
    sketch_in,
    sketch_z_out,
    sketch_z,
    sketch_t,
    gram,
    inverse,
    q_out,
    q_in,
    q_all,
    norm_near,
    norm_far,
    core_sems,
    x_sems,
    y_sems,
    gather_sems,
    sketch_sems,
    q_sems,
    near_sems,
    far_sems,
    load_sems,
    store_sems,
):
    nz, nx, ny = sizes
    z, x, y, c = (lax.axis_index(name) for name in (Z, X, Y, CORE))
    other = 1 - c
    half = summed_t.shape[1] // 2
    loads = [
        pltpu.make_async_copy(source, target, load_sems.at[i])
        for i, (source, target) in enumerate(
            (
                (momentum_in, momentum),
                (gradient_in, gradient),
                (basis_in, right_basis),
                (signs_in, signs),
                (select_in, select),
            )
        )
    ]
    for load in loads:
        load.start()
    rank = right_basis.shape[1]

    around = [{CORE: other}]
    around += [{X: lax.rem(x + d, nx)} for d in range(1, nx)]
    around += [{Y: lax.rem(y + d, ny)} for d in range(1, ny)]
    around += [{Z: lax.rem(z + d, nz)} for d in range(1, nz)]
    barrier = pltpu.get_barrier_semaphore()
    for device in around:
        pl.semaphore_signal(barrier, inc=1, device_id=device, device_id_type=MESH)

    started = []
    stores = []

    def store(source, target):
        copy = pltpu.make_async_copy(source, target, store_sems.at[len(stores)])
        copy.start()
        stores.append(copy)

    def send(source, target, sems, index, device):
        copy = pltpu.make_async_remote_copy(
            src_ref=source,
            dst_ref=target,
            send_sem=sems.at[0, index],
            recv_sem=sems.at[1, index],
            device_id=device,
            device_id_type=MESH,
        )
        copy.start()
        started.append(copy)
        return copy

    for load in loads:
        load.wait()
    summed_t[...] = momentum[...] + gradient[...].astype(jnp.float32)
    basis_t = right_basis[...].T
    away = matmul(basis_t, summed_t[:, pl.ds(pl.multiple_of(other * half, half), half)])
    part_away[...] = away.reshape(part_away.shape)
    pl.semaphore_wait(barrier, len(around))
    order = [lax.rem(x + d, nx) for d in range(1, nx)] + [x]
    core_copies = [
        send(part_away.at[to], core_in.at[to], core_sems, i, {CORE: other})
        for i, to in enumerate(order)
    ]
    store(summed_t, summed_out)
    home = matmul(basis_t, summed_t[:, pl.ds(pl.multiple_of(c * half, half), half)])
    part_home[...] = home.reshape(part_home.shape)

    x_copies = []
    for i, to in enumerate(order):
        core_copies[i].wait_recv()
        total = part_home[to] + core_in[to]
        if i < nx - 1:
            chip_sum[to] = total
            x_copies.append(send(chip_sum.at[to], x_in.at[x], x_sems, i, {X: to}))
        else:
            x_in[x] = total
    place = lax.broadcasted_iota(jnp.int32, parity.shape, 0) + (z * 2 * half + c * half)
    shared = jnp.bitwise_and(place, select[...].reshape(1, SKETCH))
    for shift in (8, 4, 2, 1):
        shared = jnp.bitwise_xor(shared, jnp.right_shift(shared, shift))
    parity[...] = 1.0 - 2.0 * jnp.bitwise_and(shared, 1).astype(jnp.float32)
    for copy in x_copies:
        copy.wait_recv()
    total = x_in[0]
    for i in range(1, nx):
        total = total + x_in[i]
    y_out[...] = total.reshape(y_out.shape)
    y_copies = []
    for d in range(1, ny):
        to = lax.rem(y + d, ny)
        y_copies.append(send(y_out.at[to], y_in.at[y], y_sems, d - 1, {Y: to}))
    y_in[y] = y_out[y]
    for copy in y_copies:
        copy.wait_recv()
    own = y_in[0]
    for i in range(1, ny):
        own = own + y_in[i]

    mine = x * ny + y

    def along_y(buffer, sems):
        copies = []
        for d in range(1, ny):
            block = buffer.at[c, mine]
            copies.append(send(block, block, sems, d - 1, {Y: lax.rem(y + d, ny)}))
        return copies

    def along_x(buffer, sems, waited):
        for copy in waited:
            copy.wait_recv()
        slab = buffer.at[c, pl.ds(x * ny, ny)]
        copies = []
        for d in range(1, nx):
            copies.append(send(slab, slab, sems, ny - 2 + d, {X: lax.rem(x + d, nx)}))
        return copies, [send(slab, slab, sems, ny + nx - 2, {CORE: other})]

    def along_core(buffer, sems, waited):
        copies = []
        for d, copy in enumerate(waited, 1):
            copy.wait_recv()
            slab = buffer.at[c, pl.ds(lax.rem(x - d + nx, nx) * ny, ny)]
            copies.append(send(slab, slab, sems, ny + nx - 2 + d, {CORE: other}))
        return copies

    left_t[c, mine] = own
    left_y = along_y(left_t, gather_sems.at[0])

    flip = signs[pl.ds(pl.multiple_of((z * 2 + c) * half, half), half)].reshape(1, half).astype(jnp.float32)
    term = matmul(own * flip, parity[...]) * (1.0 / math.sqrt(SKETCH))
    sketch_out[...] = term
    sketch_copy = send(sketch_out, sketch_in, sketch_sems, 0, {CORE: other})
    sketch_copy.wait_recv()
    term = term + sketch_in[...]
    wide = sketch_z.shape[-1]
    sketch_z_out[0] = term[:, :wide]
    sketch_z_out[1] = term[:, SKETCH - wide :]
    sketch_copies = [
        send(sketch_z_out.at[c], sketch_z.at[z], sketch_sems, d, {Z: lax.rem(z + d, nz)})
        for d in range(1, nz)
    ]
    sketch_z[z] = sketch_z_out[c]

    left_x, left_core = along_x(left_t, gather_sems.at[0], left_y)

    for copy in sketch_copies:
        copy.wait_recv()
    total = sketch_z[0]
    for i in range(1, nz):
        total = total + sketch_z[i]
    sketch_t[c, mine] = total
    sketch_y = along_y(sketch_t, gather_sems.at[1])

    left_core += along_core(left_t, gather_sems.at[0], left_x)
    for copy in left_core:
        copy.wait_recv()

    left_0 = left_t[0].reshape(rank, half)
    left_1 = left_t[1].reshape(rank, half)
    product = matmul_nt(summed_t[:, :half], left_0) + matmul_nt(summed_t[:, half:], left_1)
    q_out[...] = product.reshape(q_out.shape)
    q_copies = []
    for d in range(1, nz):
        to = lax.rem(z + d, nz)
        q_copies.append(send(q_out.at[to], q_in.at[z], q_sems, d - 1, {Z: to}))

    sketch_x, sketch_core = along_x(sketch_t, gather_sems.at[1], sketch_y)
    q_in[z] = q_out[z]
    sketch_core += along_core(sketch_t, gather_sems.at[1], sketch_x)
    for copy in sketch_core:
        copy.wait_recv()

    first = sketch_t[0].reshape(rank, wide)
    last = sketch_t[1].reshape(rank, wide)[:, 2 * wide - SKETCH :]
    gram[...] = matmul_nt(first, first) + matmul_nt(last, last)
    gathered = []
    for b in range(rank // BLOCK):
        factor_block(gram, inverse, b)
        if b == 2:
            for copy in q_copies:
                copy.wait_recv()
            total = q_in[0]
            for i in range(1, nz):
                total = total + q_in[i]
            q_all[z] = total
            for d in range(1, nz):
                block = q_all.at[z]
                to = lax.rem(z + d, nz)
                gathered.append(send(block, block, q_sems, nz - 2 + d, {Z: to}))

    share = matmul_nt(q_all[z], inverse[...])
    slot = y * 2 + c
    norm_near[slot] = jnp.sum(share * share, axis=0, keepdims=True)
    near = []
    for d in range(1, 2 * ny):
        device = {Y: lax.rem(y + d // 2, ny), CORE: lax.rem(c + d, 2)}
        near.append(send(norm_near.at[slot], norm_near.at[slot], near_sems, d, device))
    left[:, :half] = matmul(inverse[...], left_0)
    left[:, half:] = matmul(inverse[...], left_1)
    store(left, left_out)
    for copy in near:
        copy.wait_recv()
    total = norm_near[0]
    for i in range(1, 2 * ny):
        total = total + norm_near[i]
    slot = z * nx + x
    norm_far[slot] = total
    far = []
    for d in range(1, nz * nx):
        device = {Z: lax.rem(z + d // nx, nz), X: lax.rem(x + d, nx)}
        far.append(send(norm_far.at[slot], norm_far.at[slot], far_sems, d, device))
    for copy in gathered:
        copy.wait_recv()
    right[...] = matmul_nt(q_all[...].reshape(right.shape), inverse[...])
    store(right, right_out)
    for copy in far:
        copy.wait_recv()
    total = norm_far[0]
    for i in range(1, nz * nx):
        total = total + norm_far[i]
    norms[...] = jnp.sqrt(total + norm_epsilon)
    store(norms, norm_out)
    for copy in started:
        copy.wait_send()
    for copy in stores:
        copy.wait()


def split(value):
    high = value.astype(jnp.bfloat16)
    return high, (value - high.astype(jnp.float32)).astype(jnp.bfloat16)


def outputs(
    summed_in,
    left_in,
    right_in,
    norms_in,
    moved_out,
    basis_out,
    update_out,
    summed,
    left,
    right,
    norms,
    moved,
    basis,
    update,
    load_sems,
    sems,
    *,
    steps,
):
    columns, rank = right.shape
    step = columns // steps
    loads = [
        pltpu.make_async_copy(source, target, load_sems.at[i])
        for i, (source, target) in enumerate(
            ((left_in, left), (right_in, right), (norms_in, norms), (summed_in, summed))
        )
    ]
    for load in loads:
        load.start()
    loads[0].wait()
    left_high, left_low = split(left[...])
    loads[1].wait()
    loads[2].wait()
    basis[...] = right[...] / norms[...]
    copies = [pltpu.make_async_copy(basis, basis_out, sems.at[0])]
    copies[0].start()
    for i in range(steps):
        rows = pl.ds(i * step, step)
        both = jnp.concatenate([right[rows, :], basis[rows, :]], axis=0)
        high, low = split(both)
        product = jnp.dot(high, left_low, preferred_element_type=jnp.float32)
        product += jnp.dot(low, left_high, preferred_element_type=jnp.float32)
        product += jnp.dot(high, left_high, preferred_element_type=jnp.float32)
        if i == 0:
            loads[3].wait()
        moved[rows, :] = summed[rows, :] - (1.0 - decay_mu) * product[:step]
        update[rows, :] = (math.sqrt(ROWS * COLS / RANK) * product[step:]).astype(jnp.bfloat16)
        for k, (source, target) in enumerate(((moved, moved_out), (update, update_out))):
            copy = pltpu.make_async_copy(source.at[rows], target.at[rows], sems.at[1 + 2 * i + k])
            copy.start()
            copies.append(copy)
    for copy in copies:
        copy.wait()


def per_device(sizes, momentum, gradient, right_basis, signs, select):
    nz, nx, ny = sizes
    momentum, gradient = momentum.T, gradient.T
    block_cols, block_rows = momentum.shape
    rank = right_basis.shape[1]
    half = block_rows // 2
    own = rank // (nx * ny)
    wide = 256
    f32 = jnp.float32
    hbm = pl.BlockSpec(memory_space=pltpu.HBM)
    dma = pltpu.SemaphoreType.DMA
    share = block_cols // nz
    left, right, norms, summed = pl.pallas_call(
        functools.partial(factors, sizes),
        out_shape=(
            jax.ShapeDtypeStruct((rank, block_rows), f32),
            jax.ShapeDtypeStruct((block_cols, rank), f32),
            jax.ShapeDtypeStruct((1, rank), f32),
            jax.ShapeDtypeStruct((block_cols, block_rows), f32),
        ),
        in_specs=[hbm] * 5,
        out_specs=(hbm,) * 4,
        scratch_shapes=[
            pltpu.VMEM((block_cols, block_rows), f32),
            pltpu.VMEM((rank, block_rows), f32),
            pltpu.VMEM((block_cols, rank), f32),
            pltpu.VMEM((1, rank), f32),
            pltpu.VMEM((block_cols, block_rows), f32),
            pltpu.VMEM((block_cols, block_rows), jnp.bfloat16),
            pltpu.VMEM((block_cols, rank), f32),
            pltpu.VMEM((ROWS,), jnp.int32),
            pltpu.VMEM((SKETCH,), jnp.int32),
            pltpu.VMEM((nx, rank // nx, half), f32),
            pltpu.VMEM((nx, rank // nx, half), f32),
            pltpu.VMEM((nx, rank // nx, half), f32),
            pltpu.VMEM((nx, rank // nx, half), f32),
            pltpu.VMEM((nx, rank // nx, half), f32),
            pltpu.VMEM((ny, own, half), f32),
            pltpu.VMEM((ny, own, half), f32),
            pltpu.VMEM((2, nx * ny, own, half), f32),
            pltpu.VMEM((half, SKETCH), f32),
            pltpu.VMEM((own, SKETCH), f32),
            pltpu.VMEM((own, SKETCH), f32),
            pltpu.VMEM((2, own, wide), f32),
            pltpu.VMEM((nz, own, wide), f32),
            pltpu.VMEM((2, nx * ny, own, wide), f32),
            pltpu.VMEM((rank, rank), f32),
            pltpu.VMEM((rank, rank), f32),
            pltpu.VMEM((nz, share, rank), f32),
            pltpu.VMEM((nz, share, rank), f32),
            pltpu.VMEM((nz, share, rank), f32),
            pltpu.VMEM((2 * ny, 1, rank), f32),
            pltpu.VMEM((nz * nx, 1, rank), f32),
            dma((2, nx)),
            dma((2, nx)),
            dma((2, ny)),
            dma((2, 2, ny + 2 * nx)),
            dma((2, nz)),
            dma((2, 2 * nz)),
            dma((2, 2 * ny)),
            dma((2, nz * nx)),
            dma((5,)),
            dma((4,)),
        ],
        compiler_params=pltpu.CompilerParams(
            collective_id=0, has_side_effects=True, vmem_limit_bytes=64000 << 10
        ),
        name="factors",
    )(
        momentum,
        gradient,
        right_basis,
        signs,
        select,
    )
    steps = 4
    moved, basis, update = pl.pallas_call(
        functools.partial(outputs, steps=steps),
        out_shape=(
            jax.ShapeDtypeStruct((block_cols, block_rows), f32),
            jax.ShapeDtypeStruct((block_cols, rank), f32),
            jax.ShapeDtypeStruct((block_cols, block_rows), jnp.bfloat16),
        ),
        in_specs=[hbm] * 4,
        out_specs=(hbm,) * 3,
        scratch_shapes=[
            pltpu.VMEM((block_cols, block_rows), f32),
            pltpu.VMEM((rank, block_rows), f32),
            pltpu.VMEM((block_cols, rank), f32),
            pltpu.VMEM((1, rank), f32),
            pltpu.VMEM((block_cols, block_rows), f32),
            pltpu.VMEM((block_cols, rank), f32),
            pltpu.VMEM((block_cols, block_rows), jnp.bfloat16),
            dma((4,)),
            dma((1 + 2 * steps,)),
        ],
        compiler_params=pltpu.CompilerParams(vmem_limit_bytes=64000 << 10),
        name="outputs",
    )(summed, left, right, norms)
    return moved.T, basis, update.T


def solution(mesh):
    devices = mesh.devices
    shape = (mesh.shape["narrow"], 4, 8, 2) if devices.size == 512 else (2, 2, devices.size // 8, 2)
    split = Mesh(devices.reshape(shape), (Z, X, Y, CORE))
    in_specs = (P(Z, WIDE), P(Z, WIDE), P(WIDE, None), P(), P())
    out_specs = (P(Z, WIDE), P(WIDE, None), P(Z, WIDE))
    return jax.shard_map(
        functools.partial(per_device, shape[:3]),
        mesh=split,
        in_specs=in_specs,
        out_specs=out_specs,
        check_vma=False,
    )
```

```python
import functools
import math

import jax
import jax.numpy as jnp
from jax import lax
from jax.experimental import pallas as pl
from jax.experimental.pallas import tpu as pltpu
from jax.sharding import Mesh
from jax.sharding import PartitionSpec as P

ROWS = 4096
COLS = 28672
RANK = 256
SKETCH = 384
Z, X, Y, CORE = "narrow", "wide_0", "wide_1", "wide_2"
WIDE = (X, Y, CORE)
HIGH = lax.Precision.HIGHEST
MESH = pl.DeviceIdType.MESH
BLOCK = 64

decay_mu = 0.95
norm_epsilon = 1e-06


def matmul(a, b):
    return jnp.dot(a, b, precision=HIGH, preferred_element_type=jnp.float32)


def matmul_nt(a, b):
    return lax.dot_general(
        a, b, (((1,), (1,)), ((), ())), precision=HIGH, preferred_element_type=jnp.float32
    )


def matmul_tn(a, b):
    return lax.dot_general(
        a, b, (((0,), (0,)), ((), ())), precision=HIGH, preferred_element_type=jnp.float32
    )


def factor_block(a_ref, inverse_ref, b):
    n = a_ref.shape[0]
    lo, hi = b * BLOCK, (b + 1) * BLOCK
    tile, off = lo // 128, lo % 128
    lane = lax.broadcasted_iota(jnp.int32, (8, 128), 1)
    sub = lax.broadcasted_iota(jnp.int32, (8, 128), 0)
    groups = BLOCK // 8
    rows = [
        a_ref[lo + 8 * q : lo + 8 * q + 8, tile * 128 : (tile + 1) * 128] for q in range(groups)
    ]
    column = {}

    def spread(panel, first):
        for j in range(8 * panel, 8 * panel + 8):
            for q in range(first, groups):
                column[q, j] = jnp.broadcast_to(rows[q][:, off + j : off + j + 1], (8, 128))

    def row_of(value, k):
        return jnp.broadcast_to(value[k : k + 1, :], (8, 128))

    spread(0, 0)
    for p in range(groups):
        if p + 1 < groups:
            spread(p + 1, p + 1)
        for k in range(8):
            kk = 8 * p + k
            here, below = lane == off + kk, sub > k
            root = lax.rsqrt(row_of(column[p, kk], k))
            pivot = jnp.where(here, root, row_of(rows[p], k) * root)
            scaled = {q: column[q, kk] * root for q in range(p, groups)}
            scaled[p] = jnp.where(below, scaled[p], 0.0)
            for j in range(kk + 1, min(8 * (p + 2), BLOCK)):
                share = row_of(scaled[j // 8], j % 8)
                for q in range(j // 8, groups):
                    column[q, j] = column[q, j] - scaled[q] * share
            for q in range(p + 1, groups):
                rows[q] = jnp.where(here, 0.0, rows[q]) - scaled[q] * pivot
            rest = jnp.where(here & below, 0.0, rows[p]) - scaled[p] * pivot
            rows[p] = jnp.where(sub == k, pivot, rest)
    corner = jnp.concatenate(
        [
            jnp.where((lane >= off) & (lane <= off + 8 * q + sub), row, 0.0)
            for q, row in enumerate(rows)
        ],
        axis=0,
    )
    solved = matmul(corner, a_ref[tile * 128 : (tile + 1) * 128, :])
    cols = lax.broadcasted_iota(jnp.int32, (BLOCK, n), 1)
    placed = jnp.concatenate(
        [corner if t == tile else jnp.zeros_like(corner) for t in range(n // 128)], axis=1
    )
    solved = jnp.where((cols >= lo) & (cols < hi), placed, solved)
    inverse_ref[lo:hi, :] = jnp.where(cols < hi, solved, 0.0)
    if hi < n:
        start = hi // 128 * 128
        outer = matmul_tn(solved[:, start:], solved)
        cols = lax.broadcasted_iota(jnp.int32, (n - hi, n), 1)
        kept = jnp.where((cols >= lo) & (cols < hi), 0.0, a_ref[hi:n, :])
        a_ref[hi:n, :] = kept - outer[hi - start :, :]


def factors(
    sizes,
    momentum_in,
    gradient_in,
    basis_in,
    signs_in,
    select_in,
    left_out,
    right_out,
    norm_out,
    summed_out,
    summed_t,
    left,
    right,
    norms,
    momentum,
    gradient,
    right_basis,
    signs,
    select,
    part_away,
    part_home,
    core_in,
    chip_sum,
    x_in,
    y_out,
    y_in,
    left_t,
    parity,
    sketch_out,
    sketch_in,
    sketch_z_out,
    sketch_z,
    sketch_t,
    gram,
    inverse,
    q_out,
    q_in,
    q_all,
    norm_near,
    norm_far,
    core_sems,
    x_sems,
    y_sems,
    gather_sems,
    sketch_sems,
    q_sems,
    near_sems,
    far_sems,
    load_sems,
    store_sems,
):
    nz, nx, ny = sizes
    z, x, y, c = (lax.axis_index(name) for name in (Z, X, Y, CORE))
    other = 1 - c
    half = summed_t.shape[1] // 2
    loads = [
        pltpu.make_async_copy(source, target, load_sems.at[i])
        for i, (source, target) in enumerate(
            (
                (momentum_in, momentum),
                (gradient_in, gradient),
                (basis_in, right_basis),
                (signs_in, signs),
                (select_in, select),
            )
        )
    ]
    for load in loads:
        load.start()
    rank = right_basis.shape[1]

    around = [{CORE: other}]
    around += [{X: lax.rem(x + d, nx)} for d in range(1, nx)]
    around += [{Y: lax.rem(y + d, ny)} for d in range(1, ny)]
    around += [{Z: lax.rem(z + d, nz)} for d in range(1, nz)]
    barrier = pltpu.get_barrier_semaphore()
    for device in around:
        pl.semaphore_signal(barrier, inc=1, device_id=device, device_id_type=MESH)

    started = []
    stores = []

    def store(source, target):
        copy = pltpu.make_async_copy(source, target, store_sems.at[len(stores)])
        copy.start()
        stores.append(copy)

    def send(source, target, sems, index, device):
        copy = pltpu.make_async_remote_copy(
            src_ref=source,
            dst_ref=target,
            send_sem=sems.at[0, index],
            recv_sem=sems.at[1, index],
            device_id=device,
            device_id_type=MESH,
        )
        copy.start()
        started.append(copy)
        return copy

    for load in loads:
        load.wait()
    summed_t[...] = momentum[...] + gradient[...].astype(jnp.float32)
    basis_t = right_basis[...].T
    away = matmul(basis_t, summed_t[:, pl.ds(pl.multiple_of(other * half, half), half)])
    part_away[...] = away.reshape(part_away.shape)
    pl.semaphore_wait(barrier, len(around))
    order = [lax.rem(x + d, nx) for d in range(1, nx)] + [x]
    core_copies = [
        send(part_away.at[to], core_in.at[to], core_sems, i, {CORE: other})
        for i, to in enumerate(order)
    ]
    store(summed_t, summed_out)
    home = matmul(basis_t, summed_t[:, pl.ds(pl.multiple_of(c * half, half), half)])
    part_home[...] = home.reshape(part_home.shape)

    x_copies = []
    for i, to in enumerate(order):
        core_copies[i].wait_recv()
        total = part_home[to] + core_in[to]
        if i < nx - 1:
            chip_sum[to] = total
            x_copies.append(send(chip_sum.at[to], x_in.at[x], x_sems, i, {X: to}))
        else:
            x_in[x] = total
    place = lax.broadcasted_iota(jnp.int32, parity.shape, 0) + (z * 2 * half + c * half)
    shared = jnp.bitwise_and(place, select[...].reshape(1, SKETCH))
    for shift in (8, 4, 2, 1):
        shared = jnp.bitwise_xor(shared, jnp.right_shift(shared, shift))
    parity[...] = 1.0 - 2.0 * jnp.bitwise_and(shared, 1).astype(jnp.float32)
    for copy in x_copies:
        copy.wait_recv()
    total = x_in[0]
    for i in range(1, nx):
        total = total + x_in[i]
    y_out[...] = total.reshape(y_out.shape)
    y_copies = []
    for d in range(1, ny):
        to = lax.rem(y + d, ny)
        y_copies.append(send(y_out.at[to], y_in.at[y], y_sems, d - 1, {Y: to}))
    y_in[y] = y_out[y]
    for copy in y_copies:
        copy.wait_recv()
    own = y_in[0]
    for i in range(1, ny):
        own = own + y_in[i]

    mine = x * ny + y

    def along_y(buffer, sems):
        copies = []
        for d in range(1, ny):
            block = buffer.at[c, mine]
            copies.append(send(block, block, sems, d - 1, {Y: lax.rem(y + d, ny)}))
        return copies

    def along_x(buffer, sems, waited):
        copies = []
        for i, k in enumerate([0] + [k for d in range(1, ny // 2 + 1) for k in (d, ny - d)][: ny - 1]):
            if k:
                waited[k - 1].wait_recv()
            block = buffer.at[c, x * ny + lax.rem(y - k + ny, ny)]
            for d in range(1, nx):
                device = {X: lax.rem(x + d, nx)}
                copies.append(send(block, block, sems, ny - 1 + i * nx + d, device))
            if k == ny // 2:
                slab = buffer.at[c, pl.ds(x * ny, ny)]
                last = [send(slab, slab, sems, ny - 1 + i * nx, {CORE: other})]
        return copies, last

    def along_core(buffer, sems, waited):
        copies = []
        for d in range(1, nx):
            for copy in waited[d - 1 :: nx - 1]:
                copy.wait_recv()
            slab = buffer.at[c, pl.ds(lax.rem(x - d + nx, nx) * ny, ny)]
            copies.append(send(slab, slab, sems, ny - 1 + ny * nx + d, {CORE: other}))
        return copies

    left_t[c, mine] = own
    left_y = along_y(left_t, gather_sems.at[0])

    flip = signs[pl.ds(pl.multiple_of((z * 2 + c) * half, half), half)].reshape(1, half).astype(jnp.float32)
    term = matmul(own * flip, parity[...]) * (1.0 / math.sqrt(SKETCH))
    sketch_out[...] = term
    sketch_copy = send(sketch_out, sketch_in, sketch_sems, 0, {CORE: other})
    sketch_copy.wait_recv()
    term = term + sketch_in[...]
    wide = sketch_z.shape[-1]
    sketch_z_out[0] = term[:, :wide]
    sketch_z_out[1] = term[:, SKETCH - wide :]
    sketch_copies = [
        send(sketch_z_out.at[c], sketch_z.at[z], sketch_sems, d, {Z: lax.rem(z + d, nz)})
        for d in range(1, nz)
    ]
    sketch_z[z] = sketch_z_out[c]

    left_x, left_core = along_x(left_t, gather_sems.at[0], left_y)

    for copy in sketch_copies:
        copy.wait_recv()
    total = sketch_z[0]
    for i in range(1, nz):
        total = total + sketch_z[i]
    sketch_t[c, mine] = total
    sketch_y = along_y(sketch_t, gather_sems.at[1])

    left_core += along_core(left_t, gather_sems.at[0], left_x)
    for copy in left_core:
        copy.wait_recv()

    left_0 = left_t[0].reshape(rank, half)
    left_1 = left_t[1].reshape(rank, half)
    product = matmul_nt(summed_t[:, :half], left_0) + matmul_nt(summed_t[:, half:], left_1)
    q_out[...] = product.reshape(q_out.shape)
    q_copies = []
    for d in range(1, nz):
        to = lax.rem(z + d, nz)
        q_copies.append(send(q_out.at[to], q_in.at[z], q_sems, d - 1, {Z: to}))

    sketch_x, sketch_core = along_x(sketch_t, gather_sems.at[1], sketch_y)
    q_in[z] = q_out[z]
    sketch_core += along_core(sketch_t, gather_sems.at[1], sketch_x)
    for copy in sketch_core:
        copy.wait_recv()

    first = sketch_t[0].reshape(rank, wide)
    last = sketch_t[1].reshape(rank, wide)[:, 2 * wide - SKETCH :]
    gram[...] = matmul_nt(first, first) + matmul_nt(last, last)
    gathered = []
    for b in range(rank // BLOCK):
        factor_block(gram, inverse, b)
        if b == rank // BLOCK // 2 - 1:
            for copy in q_copies:
                copy.wait_recv()
            total = q_in[0]
            for i in range(1, nz):
                total = total + q_in[i]
            q_all[z] = total
            for d in range(1, nz):
                block = q_all.at[z]
                to = lax.rem(z + d, nz)
                gathered.append(send(block, block, q_sems, nz - 2 + d, {Z: to}))

    share = matmul_nt(q_all[z], inverse[...])
    slot = y * 2 + c
    norm_near[slot] = jnp.sum(share * share, axis=0, keepdims=True)
    near = []
    for d in range(1, 2 * ny):
        device = {Y: lax.rem(y + d // 2, ny), CORE: lax.rem(c + d, 2)}
        near.append(send(norm_near.at[slot], norm_near.at[slot], near_sems, d, device))
    left[:, :half] = matmul(inverse[...], left_0)
    left[:, half:] = matmul(inverse[...], left_1)
    store(left, left_out)
    for copy in near:
        copy.wait_recv()
    total = norm_near[0]
    for i in range(1, 2 * ny):
        total = total + norm_near[i]
    slot = z * nx + x
    norm_far[slot] = total
    far = []
    for d in range(1, nz * nx):
        device = {Z: lax.rem(z + d // nx, nz), X: lax.rem(x + d, nx)}
        far.append(send(norm_far.at[slot], norm_far.at[slot], far_sems, d, device))
    for copy in gathered:
        copy.wait_recv()
    right[...] = matmul_nt(q_all[...].reshape(right.shape), inverse[...])
    store(right, right_out)
    for copy in far:
        copy.wait_recv()
    total = norm_far[0]
    for i in range(1, nz * nx):
        total = total + norm_far[i]
    norms[...] = jnp.sqrt(total + norm_epsilon)
    store(norms, norm_out)
    for copy in started:
        copy.wait_send()
    for copy in stores:
        copy.wait()


def split(value):
    high = value.astype(jnp.bfloat16)
    return high, (value - high.astype(jnp.float32)).astype(jnp.bfloat16)


def outputs(
    summed_in,
    left_in,
    right_in,
    norms_in,
    moved_out,
    basis_out,
    update_out,
    summed,
    left,
    right,
    norms,
    moved,
    basis,
    update,
    load_sems,
    sems,
    *,
    steps,
):
    columns, rank = right.shape
    step = columns // steps
    loads = [
        pltpu.make_async_copy(source, target, load_sems.at[i])
        for i, (source, target) in enumerate(
            ((left_in, left), (right_in, right), (norms_in, norms), (summed_in, summed))
        )
    ]
    for load in loads:
        load.start()
    loads[0].wait()
    left_high, left_low = split(left[...])
    loads[1].wait()
    loads[2].wait()
    basis[...] = right[...] / norms[...]
    copies = [pltpu.make_async_copy(basis, basis_out, sems.at[0])]
    copies[0].start()
    for i in range(steps):
        rows = pl.ds(i * step, step)
        both = jnp.concatenate([right[rows, :], basis[rows, :]], axis=0)
        high, low = split(both)
        product = jnp.dot(high, left_low, preferred_element_type=jnp.float32)
        product += jnp.dot(low, left_high, preferred_element_type=jnp.float32)
        product += jnp.dot(high, left_high, preferred_element_type=jnp.float32)
        if i == 0:
            loads[3].wait()
        moved[rows, :] = summed[rows, :] - (1.0 - decay_mu) * product[:step]
        update[rows, :] = (math.sqrt(ROWS * COLS / RANK) * product[step:]).astype(jnp.bfloat16)
        for k, (source, target) in enumerate(((moved, moved_out), (update, update_out))):
            copy = pltpu.make_async_copy(source.at[rows], target.at[rows], sems.at[1 + 2 * i + k])
            copy.start()
            copies.append(copy)
    for copy in copies:
        copy.wait()


def per_device(sizes, momentum, gradient, right_basis, signs, select):
    nz, nx, ny = sizes
    momentum, gradient = momentum.T, gradient.T
    block_cols, block_rows = momentum.shape
    rank = right_basis.shape[1]
    half = block_rows // 2
    own = rank // (nx * ny)
    wide = 256
    f32 = jnp.float32
    hbm = pl.BlockSpec(memory_space=pltpu.HBM)
    dma = pltpu.SemaphoreType.DMA
    share = block_cols // nz
    left, right, norms, summed = pl.pallas_call(
        functools.partial(factors, sizes),
        out_shape=(
            jax.ShapeDtypeStruct((rank, block_rows), f32),
            jax.ShapeDtypeStruct((block_cols, rank), f32),
            jax.ShapeDtypeStruct((1, rank), f32),
            jax.ShapeDtypeStruct((block_cols, block_rows), f32),
        ),
        in_specs=[hbm] * 5,
        out_specs=(hbm,) * 4,
        scratch_shapes=[
            pltpu.VMEM((block_cols, block_rows), f32),
            pltpu.VMEM((rank, block_rows), f32),
            pltpu.VMEM((block_cols, rank), f32),
            pltpu.VMEM((1, rank), f32),
            pltpu.VMEM((block_cols, block_rows), f32),
            pltpu.VMEM((block_cols, block_rows), jnp.bfloat16),
            pltpu.VMEM((block_cols, rank), f32),
            pltpu.VMEM((ROWS,), jnp.int32),
            pltpu.VMEM((SKETCH,), jnp.int32),
            pltpu.VMEM((nx, rank // nx, half), f32),
            pltpu.VMEM((nx, rank // nx, half), f32),
            pltpu.VMEM((nx, rank // nx, half), f32),
            pltpu.VMEM((nx, rank // nx, half), f32),
            pltpu.VMEM((nx, rank // nx, half), f32),
            pltpu.VMEM((ny, own, half), f32),
            pltpu.VMEM((ny, own, half), f32),
            pltpu.VMEM((2, nx * ny, own, half), f32),
            pltpu.VMEM((half, SKETCH), f32),
            pltpu.VMEM((own, SKETCH), f32),
            pltpu.VMEM((own, SKETCH), f32),
            pltpu.VMEM((2, own, wide), f32),
            pltpu.VMEM((nz, own, wide), f32),
            pltpu.VMEM((2, nx * ny, own, wide), f32),
            pltpu.VMEM((rank, rank), f32),
            pltpu.VMEM((rank, rank), f32),
            pltpu.VMEM((nz, share, rank), f32),
            pltpu.VMEM((nz, share, rank), f32),
            pltpu.VMEM((nz, share, rank), f32),
            pltpu.VMEM((2 * ny, 1, rank), f32),
            pltpu.VMEM((nz * nx, 1, rank), f32),
            dma((2, nx)),
            dma((2, nx)),
            dma((2, ny)),
            dma((2, 2, ny + (ny + 1) * nx)),
            dma((2, nz)),
            dma((2, 2 * nz)),
            dma((2, 2 * ny)),
            dma((2, nz * nx)),
            dma((5,)),
            dma((4,)),
        ],
        compiler_params=pltpu.CompilerParams(
            collective_id=0, has_side_effects=True, vmem_limit_bytes=64000 << 10
        ),
        name="factors",
    )(
        momentum,
        gradient,
        right_basis,
        signs,
        select,
    )
    steps = 4
    moved, basis, update = pl.pallas_call(
        functools.partial(outputs, steps=steps),
        out_shape=(
            jax.ShapeDtypeStruct((block_cols, block_rows), f32),
            jax.ShapeDtypeStruct((block_cols, rank), f32),
            jax.ShapeDtypeStruct((block_cols, block_rows), jnp.bfloat16),
        ),
        in_specs=[hbm] * 4,
        out_specs=(hbm,) * 3,
        scratch_shapes=[
            pltpu.VMEM((block_cols, block_rows), f32),
            pltpu.VMEM((rank, block_rows), f32),
            pltpu.VMEM((block_cols, rank), f32),
            pltpu.VMEM((1, rank), f32),
            pltpu.VMEM((block_cols, block_rows), f32),
            pltpu.VMEM((block_cols, rank), f32),
            pltpu.VMEM((block_cols, block_rows), jnp.bfloat16),
            dma((4,)),
            dma((1 + 2 * steps,)),
        ],
        compiler_params=pltpu.CompilerParams(vmem_limit_bytes=64000 << 10),
        name="outputs",
    )(summed, left, right, norms)
    return moved.T, basis, update.T


def solution(mesh):
    devices = mesh.devices
    shape = (mesh.shape["narrow"], 4, 8, 2) if devices.size == 512 else (2, 2, devices.size // 8, 2)
    split = Mesh(devices.reshape(shape), (Z, X, Y, CORE))
    in_specs = (P(Z, WIDE), P(Z, WIDE), P(WIDE, None), P(), P())
    out_specs = (P(Z, WIDE), P(WIDE, None), P(Z, WIDE))
    return jax.shard_map(
        functools.partial(per_device, shape[:3]),
        mesh=split,
        in_specs=in_specs,
        out_specs=out_specs,
        check_vma=False,
    )
```

```python
import functools
import math

import jax
import jax.numpy as jnp
from jax import lax
from jax.experimental import pallas as pl
from jax.experimental.pallas import tpu as pltpu
from jax.sharding import Mesh
from jax.sharding import PartitionSpec as P

ROWS = 4096
COLS = 28672
RANK = 256
SKETCH = 384
Z, X, Y, CORE = "narrow", "wide_0", "wide_1", "wide_2"
WIDE = (X, Y, CORE)
HIGH = lax.Precision.HIGHEST
MESH = pl.DeviceIdType.MESH
BLOCK = 64

decay_mu = 0.95
norm_epsilon = 1e-06


def matmul(a, b):
    return jnp.dot(a, b, precision=HIGH, preferred_element_type=jnp.float32)


def matmul_nt(a, b):
    return lax.dot_general(
        a, b, (((1,), (1,)), ((), ())), precision=HIGH, preferred_element_type=jnp.float32
    )


def matmul_tn(a, b):
    return lax.dot_general(
        a, b, (((0,), (0,)), ((), ())), precision=HIGH, preferred_element_type=jnp.float32
    )


def factor_block(a_ref, inverse_ref, b):
    n = a_ref.shape[0]
    lo, hi = b * BLOCK, (b + 1) * BLOCK
    tile, off = lo // 128, lo % 128
    lane = lax.broadcasted_iota(jnp.int32, (8, 128), 1)
    sub = lax.broadcasted_iota(jnp.int32, (8, 128), 0)
    groups = BLOCK // 8
    rows = [
        a_ref[lo + 8 * q : lo + 8 * q + 8, tile * 128 : (tile + 1) * 128] for q in range(groups)
    ]
    column = {}

    def spread(panel, first):
        for j in range(8 * panel, 8 * panel + 8):
            for q in range(first, groups):
                column[q, j] = jnp.broadcast_to(rows[q][:, off + j : off + j + 1], (8, 128))

    def row_of(value, k):
        return jnp.broadcast_to(value[k : k + 1, :], (8, 128))

    spread(0, 0)
    for p in range(groups):
        if p + 1 < groups:
            spread(p + 1, p + 1)
        for k in range(8):
            kk = 8 * p + k
            here, below = lane == off + kk, sub > k
            root = lax.rsqrt(row_of(column[p, kk], k))
            pivot = jnp.where(here, root, row_of(rows[p], k) * root)
            scaled = {q: column[q, kk] * root for q in range(p, groups)}
            scaled[p] = jnp.where(below, scaled[p], 0.0)
            for j in range(kk + 1, min(8 * (p + 2), BLOCK)):
                share = row_of(scaled[j // 8], j % 8)
                for q in range(j // 8, groups):
                    column[q, j] = column[q, j] - scaled[q] * share
            for q in range(p + 1, groups):
                rows[q] = jnp.where(here, 0.0, rows[q]) - scaled[q] * pivot
            rest = jnp.where(here & below, 0.0, rows[p]) - scaled[p] * pivot
            rows[p] = jnp.where(sub == k, pivot, rest)
    corner = jnp.concatenate(
        [
            jnp.where((lane >= off) & (lane <= off + 8 * q + sub), row, 0.0)
            for q, row in enumerate(rows)
        ],
        axis=0,
    )
    solved = matmul(corner, a_ref[tile * 128 : (tile + 1) * 128, :])
    cols = lax.broadcasted_iota(jnp.int32, (BLOCK, n), 1)
    placed = jnp.concatenate(
        [corner if t == tile else jnp.zeros_like(corner) for t in range(n // 128)], axis=1
    )
    solved = jnp.where((cols >= lo) & (cols < hi), placed, solved)
    inverse_ref[lo:hi, :] = jnp.where(cols < hi, solved, 0.0)
    if hi < n:
        start = hi // 128 * 128
        outer = matmul_tn(solved[:, start:], solved)
        cols = lax.broadcasted_iota(jnp.int32, (n - hi, n), 1)
        kept = jnp.where((cols >= lo) & (cols < hi), 0.0, a_ref[hi:n, :])
        a_ref[hi:n, :] = kept - outer[hi - start :, :]


def factors(
    sizes,
    momentum_in,
    gradient_in,
    basis_in,
    signs_in,
    select_in,
    left_out,
    right_out,
    norm_out,
    summed_t,
    basis_t,
    momentum,
    gradient,
    right_basis,
    signs,
    select,
    part_away,
    part_home,
    core_in,
    chip_sum,
    x_in,
    y_out,
    y_in,
    left_t,
    left_full,
    parity,
    sketch_z_out,
    sketch_z,
    sketch_t,
    sketch_full,
    gram,
    inverse,
    q_out,
    q_in,
    q_all,
    norm_near,
    norm_far,
    core_sems,
    x_sems,
    y_sems,
    gather_sems,
    sketch_sems,
    q_sems,
    near_sems,
    far_sems,
    load_sems,
):
    nz, nx, ny = sizes
    z, x, y, c = (lax.axis_index(name) for name in (Z, X, Y, CORE))
    other = 1 - c
    half = summed_t.shape[1] // 2
    loads = [
        pltpu.make_async_copy(source, target, load_sems.at[i])
        for i, (source, target) in enumerate(
            (
                (momentum_in, momentum),
                (gradient_in, gradient),
                (basis_in, right_basis),
                (signs_in, signs),
                (select_in, select),
            )
        )
    ]
    for load in loads:
        load.start()
    rank = right_basis.shape[1]

    around = [{CORE: other}]
    around += [{X: lax.rem(x + d, nx)} for d in range(1, nx)]
    around += [{Y: lax.rem(y + d, ny)} for d in range(1, ny)]
    around += [{Z: lax.rem(z + d, nz)} for d in range(1, nz)]
    barrier = pltpu.get_barrier_semaphore()
    for device in around:
        pl.semaphore_signal(barrier, inc=1, device_id=device, device_id_type=MESH)

    started = []

    def send(source, target, sems, index, device):
        copy = pltpu.make_async_remote_copy(
            src_ref=source,
            dst_ref=target,
            send_sem=sems.at[0, index],
            recv_sem=sems.at[1, index],
            device_id=device,
            device_id_type=MESH,
        )
        copy.start()
        started.append(copy)
        return copy

    for load in loads:
        load.wait()
    summed_t[...] = momentum[...] + gradient[...].astype(jnp.float32)
    basis_t[...] = right_basis[...].T
    rows = rank // 2
    away = matmul(basis_t[pl.ds(pl.multiple_of(other * rows, rows), rows), :], summed_t[...])
    part_away[...] = away.reshape(part_away.shape)
    pl.semaphore_wait(barrier, len(around))
    order = [lax.rem(x + d, nx) for d in sorted(range(1, nx), key=lambda d: -min(d, nx - d))] + [x]
    core_copies = [
        send(part_away.at[to], core_in.at[to], core_sems, i, {CORE: other})
        for i, to in enumerate(order)
    ]
    home = matmul(basis_t[pl.ds(pl.multiple_of(c * rows, rows), rows), :], summed_t[...])
    part_home[...] = home.reshape(part_home.shape)

    x_copies = []
    for i, to in enumerate(order):
        core_copies[i].wait_recv()
        total = part_home[to] + core_in[to]
        if i < nx - 1:
            chip_sum[to] = total
            x_copies.append(send(chip_sum.at[to], x_in.at[x], x_sems, i, {X: to}))
        else:
            x_in[x] = total
    place = lax.broadcasted_iota(jnp.int32, parity.shape, 0) + z * 2 * half
    shared = jnp.bitwise_and(place, select[...].reshape(1, SKETCH))
    for shift in (8, 4, 2, 1):
        shared = jnp.bitwise_xor(shared, jnp.right_shift(shared, shift))
    parity[...] = 1.0 - 2.0 * jnp.bitwise_and(shared, 1).astype(jnp.float32)
    for copy in x_copies:
        copy.wait_recv()
    total = x_in[0]
    for i in range(1, nx):
        total = total + x_in[i]
    own_rows = total.shape[0] // ny
    for i in range(ny):
        part = total[i * own_rows : (i + 1) * own_rows]
        y_out[i] = jnp.concatenate([part[:, :half], part[:, half:]], axis=0)
    y_copies = []
    for d in range(1, ny):
        to = lax.rem(y + d, ny)
        y_copies.append(send(y_out.at[to], y_in.at[y], y_sems, d - 1, {Y: to}))
    y_in[y] = y_out[y]
    for copy in y_copies:
        copy.wait_recv()
    own = y_in[0]
    for i in range(1, ny):
        own = own + y_in[i]

    mine = x * ny + y

    def along_y(buffer, sems):
        copies = []
        for d in range(1, ny):
            block = buffer.at[c, mine]
            copies.append(send(block, block, sems, d - 1, {Y: lax.rem(y + d, ny)}))
        return copies

    def along_x(buffer, sems, waited):
        copies = []
        for i, k in enumerate([0] + [k for d in range(1, ny // 2 + 1) for k in (d, ny - d)][: ny - 1]):
            if k:
                waited[k - 1].wait_recv()
            block = buffer.at[c, x * ny + lax.rem(y - k + ny, ny)]
            for d in range(1, nx):
                device = {X: lax.rem(x + d, nx)}
                copies.append(send(block, block, sems, ny - 1 + i * nx + d, device))
            if k == ny // 2:
                slab = buffer.at[c, pl.ds(x * ny, ny)]
                last = [send(slab, slab, sems, ny - 1 + i * nx, {CORE: other})]
        return copies, last

    def along_core(buffer, sems, waited):
        copies = []
        for d in range(1, nx):
            for copy in waited[d - 1 :: nx - 1]:
                copy.wait_recv()
            slab = buffer.at[c, pl.ds(lax.rem(x - d + nx, nx) * ny, ny)]
            copies.append(send(slab, slab, sems, ny - 1 + ny * nx + d, {CORE: other}))
        return copies

    def unpacked(buffer):
        pieces = []
        for core in range(2):
            for i in range(0, nx * ny, 2):
                a, b = buffer[core, i], buffer[core, i + 1]
                start = core * rows + i * own_rows
                low = jnp.concatenate([a[:own_rows], b[:own_rows]], axis=0)
                high = jnp.concatenate([a[own_rows:], b[own_rows:]], axis=0)
                pieces.append((slice(start, start + 2 * own_rows), low, high))
        return pieces

    left_t[c, mine] = own
    left_y = along_y(left_t, gather_sems.at[0])

    flip = signs[pl.ds(pl.multiple_of(z * 2 * half, 2 * half), 2 * half)]
    flip = flip.reshape(1, 2 * half).astype(jnp.float32)
    low = matmul(own * flip[:, :half], parity[:half, :])
    high = matmul(own * flip[:, half:], parity[half:, :])
    term = (low[:own_rows] + high[own_rows:]) * (1.0 / math.sqrt(SKETCH))
    wide = sketch_z.shape[-1]
    sketch_z_out[...] = jnp.concatenate([term[:, :wide], term[:, SKETCH - wide :]], axis=0)
    sketch_copies = [
        send(sketch_z_out, sketch_z.at[z], sketch_sems, d, {Z: lax.rem(z + d, nz)})
        for d in range(1, nz)
    ]
    sketch_z[z] = sketch_z_out[...]

    left_x, left_core = along_x(left_t, gather_sems.at[0], left_y)

    for copy in sketch_copies:
        copy.wait_recv()
    total = sketch_z[0]
    for i in range(1, nz):
        total = total + sketch_z[i]
    sketch_t[c, mine] = total
    sketch_y = along_y(sketch_t, gather_sems.at[1])

    left_core += along_core(left_t, gather_sems.at[0], left_x)
    for copy in left_core:
        copy.wait_recv()

    for top, low, high in unpacked(left_t):
        left_full[top, :half] = low
        left_full[top, half:] = high
    product = matmul_nt(summed_t[...], left_full[...])
    q_out[...] = product.reshape(q_out.shape)
    q_copies = []
    for d in range(1, nz):
        to = lax.rem(z + d, nz)
        q_copies.append(send(q_out.at[to], q_in.at[z], q_sems, d - 1, {Z: to}))

    sketch_x, sketch_core = along_x(sketch_t, gather_sems.at[1], sketch_y)
    q_in[z] = q_out[z]
    sketch_core += along_core(sketch_t, gather_sems.at[1], sketch_x)
    for copy in sketch_core:
        copy.wait_recv()

    for top, low, high in unpacked(sketch_t):
        sketch_full[top, :wide] = low
        sketch_full[top, wide:] = high[:, 2 * wide - SKETCH :]
    gram[...] = matmul_nt(sketch_full[...], sketch_full[...])
    gathered = []
    for b in range(rank // BLOCK):
        factor_block(gram, inverse, b)
        if b == 0:
            for copy in q_copies:
                copy.wait_recv()
            total = q_in[0]
            for i in range(1, nz):
                total = total + q_in[i]
            q_all[z] = total
            for d in range(1, nz):
                block = q_all.at[z]
                to = lax.rem(z + d, nz)
                gathered.append(send(block, block, q_sems, nz - 2 + d, {Z: to}))

    share = matmul_nt(q_all[z], inverse[...])
    slot = y * 2 + c
    norm_near[slot] = jnp.sum(share * share, axis=0, keepdims=True)
    near = []
    for d in range(1, 2 * ny):
        device = {Y: lax.rem(y + d // 2, ny), CORE: lax.rem(c + d, 2)}
        near.append(send(norm_near.at[slot], norm_near.at[slot], near_sems, d, device))
    left_out[...] = matmul(inverse[...], left_full[...])
    for copy in near:
        copy.wait_recv()
    total = norm_near[0]
    for i in range(1, 2 * ny):
        total = total + norm_near[i]
    slot = z * nx + x
    norm_far[slot] = total
    far = []
    for d in range(1, nz * nx):
        device = {Z: lax.rem(z + d // nx, nz), X: lax.rem(x + d, nx)}
        far.append(send(norm_far.at[slot], norm_far.at[slot], far_sems, d, device))
    for copy in gathered:
        copy.wait_recv()
    right_out[...] = matmul_nt(q_all[...].reshape(right_out.shape), inverse[...])
    for copy in far:
        copy.wait_recv()
    total = norm_far[0]
    for i in range(1, nz * nx):
        total = total + norm_far[i]
    norm_out[...] = jnp.sqrt(total + norm_epsilon)
    for copy in started:
        copy.wait_send()


def split(value):
    high = value.astype(jnp.bfloat16)
    return high, (value - high.astype(jnp.float32)).astype(jnp.bfloat16)


def outputs(
    summed,
    left,
    right,
    norms,
    moved_out,
    basis_out,
    update_out,
    moved,
    basis,
    update,
    sems,
    *,
    steps,
):
    columns, rank = right.shape
    step = columns // steps
    left_high, left_low = split(left[...])
    basis[...] = right[...] / norms[...]
    copies = [pltpu.make_async_copy(basis, basis_out, sems.at[0])]
    copies[0].start()
    for i in range(steps):
        rows = pl.ds(i * step, step)
        both = jnp.concatenate([right[rows, :], basis[rows, :]], axis=0)
        high, low = split(both)
        product = jnp.dot(high, left_low, preferred_element_type=jnp.float32)
        product += jnp.dot(low, left_high, preferred_element_type=jnp.float32)
        product += jnp.dot(high, left_high, preferred_element_type=jnp.float32)
        moved[rows, :] = summed[rows, :] - (1.0 - decay_mu) * product[:step]
        update[rows, :] = (math.sqrt(ROWS * COLS / RANK) * product[step:]).astype(jnp.bfloat16)
        for k, (source, target) in enumerate(((moved, moved_out), (update, update_out))):
            copy = pltpu.make_async_copy(source.at[rows], target.at[rows], sems.at[1 + 2 * i + k])
            copy.start()
            copies.append(copy)
    for copy in copies:
        copy.wait()


def per_device(sizes, momentum, gradient, right_basis, signs, select):
    nz, nx, ny = sizes
    momentum, gradient, right_basis, signs, select = (
        pltpu.with_memory_space_constraint(value, pltpu.HBM)
        for value in (momentum.T, gradient.T, right_basis, signs, select)
    )
    block_cols, block_rows = momentum.shape
    rank = right_basis.shape[1]
    half = block_rows // 2
    own = 2 * rank // (2 * nx * ny)
    wide = 256
    f32 = jnp.float32
    vmem = pl.BlockSpec(memory_space=pltpu.VMEM)
    hbm = pl.BlockSpec(memory_space=pltpu.HBM)
    dma = pltpu.SemaphoreType.DMA
    share = block_cols // nz
    left, right, norms, summed = pl.pallas_call(
        functools.partial(factors, sizes),
        out_shape=(
            jax.ShapeDtypeStruct((rank, block_rows), f32),
            jax.ShapeDtypeStruct((block_cols, rank), f32),
            jax.ShapeDtypeStruct((1, rank), f32),
            jax.ShapeDtypeStruct((block_cols, block_rows), f32),
        ),
        in_specs=[hbm] * 5,
        out_specs=(vmem,) * 4,
        scratch_shapes=[
            pltpu.VMEM((rank, block_cols), f32),
            pltpu.VMEM((block_cols, block_rows), f32),
            pltpu.VMEM((block_cols, block_rows), jnp.bfloat16),
            pltpu.VMEM((block_cols, rank), f32),
            pltpu.VMEM((ROWS,), jnp.int32),
            pltpu.VMEM((SKETCH,), jnp.int32),
            pltpu.VMEM((nx, rank // (2 * nx), block_rows), f32),
            pltpu.VMEM((nx, rank // (2 * nx), block_rows), f32),
            pltpu.VMEM((nx, rank // (2 * nx), block_rows), f32),
            pltpu.VMEM((nx, rank // (2 * nx), block_rows), f32),
            pltpu.VMEM((nx, rank // (2 * nx), block_rows), f32),
            pltpu.VMEM((ny, own, half), f32),
            pltpu.VMEM((ny, own, half), f32),
            pltpu.VMEM((2, nx * ny, own, half), f32),
            pltpu.VMEM((rank, block_rows), f32),
            pltpu.VMEM((block_rows, SKETCH), f32),
            pltpu.VMEM((own, wide), f32),
            pltpu.VMEM((nz, own, wide), f32),
            pltpu.VMEM((2, nx * ny, own, wide), f32),
            pltpu.VMEM((rank, SKETCH), f32),
            pltpu.VMEM((rank, rank), f32),
            pltpu.VMEM((rank, rank), f32),
            pltpu.VMEM((nz, share, rank), f32),
            pltpu.VMEM((nz, share, rank), f32),
            pltpu.VMEM((nz, share, rank), f32),
            pltpu.VMEM((2 * ny, 1, rank), f32),
            pltpu.VMEM((nz * nx, 1, rank), f32),
            dma((2, nx)),
            dma((2, nx)),
            dma((2, ny)),
            dma((2, 2, ny + (ny + 1) * nx)),
            dma((2, nz)),
            dma((2, 2 * nz)),
            dma((2, 2 * ny)),
            dma((2, nz * nx)),
            dma((5,)),
        ],
        compiler_params=pltpu.CompilerParams(
            collective_id=0, has_side_effects=True, vmem_limit_bytes=40 << 20
        ),
        name="factors",
    )(
        momentum,
        gradient,
        right_basis,
        signs,
        select,
    )
    steps = 4
    moved, basis, update = pl.pallas_call(
        functools.partial(outputs, steps=steps),
        out_shape=(
            jax.ShapeDtypeStruct((block_cols, block_rows), f32),
            jax.ShapeDtypeStruct((block_cols, rank), f32),
            jax.ShapeDtypeStruct((block_cols, block_rows), jnp.bfloat16),
        ),
        in_specs=[vmem] * 4,
        out_specs=(hbm,) * 3,
        scratch_shapes=[
            pltpu.VMEM((block_cols, block_rows), f32),
            pltpu.VMEM((block_cols, rank), f32),
            pltpu.VMEM((block_cols, block_rows), jnp.bfloat16),
            dma((1 + 2 * steps,)),
        ],
        compiler_params=pltpu.CompilerParams(vmem_limit_bytes=20 << 20),
        name="outputs",
    )(summed, left, right, norms)
    return moved.T, basis, update.T


def solution(mesh):
    devices = mesh.devices
    shape = (mesh.shape["narrow"], 4, 8, 2) if devices.size == 512 else (2, 2, devices.size // 8, 2)
    split = Mesh(devices.reshape(shape), (Z, X, Y, CORE))
    in_specs = (P(Z, WIDE), P(Z, WIDE), P(WIDE, None), P(), P())
    out_specs = (P(Z, WIDE), P(WIDE, None), P(Z, WIDE))
    return jax.shard_map(
        functools.partial(per_device, shape[:3]),
        mesh=split,
        in_specs=in_specs,
        out_specs=out_specs,
        check_vma=False,
    )
```

```python
import functools
import math

import jax
import jax.numpy as jnp
from jax import lax
from jax.experimental import pallas as pl
from jax.experimental.pallas import tpu as pltpu
from jax.sharding import Mesh
from jax.sharding import PartitionSpec as P

ROWS = 4096
COLS = 28672
RANK = 256
SKETCH = 384
Z, X, Y, CORE = "narrow", "wide_0", "wide_1", "wide_2"
WIDE = (X, Y, CORE)
HIGH = lax.Precision.HIGHEST
MESH = pl.DeviceIdType.MESH
BLOCK = 64

decay_mu = 0.95
norm_epsilon = 1e-06


def matmul(a, b):
    return jnp.dot(a, b, precision=HIGH, preferred_element_type=jnp.float32)


def matmul_nt(a, b):
    return lax.dot_general(
        a, b, (((1,), (1,)), ((), ())), precision=HIGH, preferred_element_type=jnp.float32
    )


def matmul_tn(a, b):
    return lax.dot_general(
        a, b, (((0,), (0,)), ((), ())), precision=HIGH, preferred_element_type=jnp.float32
    )


def sign_product(value, signs):
    rows = value.shape[0]
    pieces = []
    for _ in range(3):
        pieces.append(value.astype(jnp.bfloat16).astype(jnp.float32))
        value = value - pieces[-1]
    stacked = jnp.concatenate(pieces, axis=0).astype(jnp.bfloat16)
    product = jnp.dot(stacked, signs, preferred_element_type=jnp.float32)
    return product[:rows] + product[rows : 2 * rows] + product[2 * rows :]


def factor_block(a_ref, inverse_ref, b):
    n = a_ref.shape[0]
    lo, hi = b * BLOCK, (b + 1) * BLOCK
    tile, off = lo // 128, lo % 128
    lane = lax.broadcasted_iota(jnp.int32, (8, 128), 1)
    sub = lax.broadcasted_iota(jnp.int32, (8, 128), 0)
    groups = BLOCK // 8
    rows = [
        a_ref[lo + 8 * q : lo + 8 * q + 8, tile * 128 : (tile + 1) * 128] for q in range(groups)
    ]
    column = {}

    def spread(panel, first):
        for j in range(8 * panel, 8 * panel + 8):
            for q in range(first, groups):
                column[q, j] = jnp.broadcast_to(rows[q][:, off + j : off + j + 1], (8, 128))

    def row_of(value, k):
        return jnp.broadcast_to(value[k : k + 1, :], (8, 128))

    spread(0, 0)
    for p in range(groups):
        if p + 1 < groups:
            spread(p + 1, p + 1)
        for k in range(8):
            kk = 8 * p + k
            here, below = lane == off + kk, sub > k
            root = lax.rsqrt(row_of(column[p, kk], k))
            pivot = jnp.where(here, root, row_of(rows[p], k) * root)
            scaled = {q: column[q, kk] * root for q in range(p, groups)}
            scaled[p] = jnp.where(below, scaled[p], 0.0)
            for j in range(kk + 1, min(8 * (p + 2), BLOCK)):
                share = row_of(scaled[j // 8], j % 8)
                for q in range(j // 8, groups):
                    column[q, j] = column[q, j] - scaled[q] * share
            for q in range(p + 1, groups):
                rows[q] = jnp.where(here, 0.0, rows[q]) - scaled[q] * pivot
            rest = jnp.where(here & below, 0.0, rows[p]) - scaled[p] * pivot
            rows[p] = jnp.where(sub == k, pivot, rest)
    corner = jnp.concatenate(
        [
            jnp.where((lane >= off) & (lane <= off + 8 * q + sub), row, 0.0)
            for q, row in enumerate(rows)
        ],
        axis=0,
    )
    solved = matmul(corner, a_ref[tile * 128 : (tile + 1) * 128, :])
    cols = lax.broadcasted_iota(jnp.int32, (BLOCK, n), 1)
    placed = jnp.concatenate(
        [corner if t == tile else jnp.zeros_like(corner) for t in range(n // 128)], axis=1
    )
    solved = jnp.where((cols >= lo) & (cols < hi), placed, solved)
    inverse_ref[lo:hi, :] = jnp.where(cols < hi, solved, 0.0)
    if hi < n:
        start = hi // 128 * 128
        outer = matmul_tn(solved[:, start:], solved)
        cols = lax.broadcasted_iota(jnp.int32, (n - hi, n), 1)
        kept = jnp.where((cols >= lo) & (cols < hi), 0.0, a_ref[hi:n, :])
        a_ref[hi:n, :] = kept - outer[hi - start :, :]


def factors(
    sizes,
    momentum_in,
    gradient_in,
    basis_in,
    signs_in,
    select_in,
    left_out,
    right_out,
    norm_out,
    summed_t,
    basis_t,
    momentum,
    gradient,
    right_basis,
    signs,
    select,
    part_away,
    part_home,
    core_in,
    chip_sum,
    x_in,
    y_out,
    y_in,
    left_t,
    left_full,
    parity,
    sketch_z_out,
    sketch_z,
    sketch_t,
    sketch_full,
    gram,
    inverse,
    q_out,
    q_in,
    q_relay,
    q_all,
    norm_near,
    norm_far,
    core_sems,
    x_sems,
    y_sems,
    gather_sems,
    sketch_sems,
    q_sems,
    near_sems,
    far_sems,
    load_sems,
):
    nz, nx, ny = sizes
    z, x, y, c = (lax.axis_index(name) for name in (Z, X, Y, CORE))
    other = 1 - c
    half = summed_t.shape[1] // 2
    loads = [
        pltpu.make_async_copy(source, target, load_sems.at[i])
        for i, (source, target) in enumerate(
            (
                (momentum_in, momentum),
                (gradient_in, gradient),
                (basis_in, right_basis),
                (signs_in, signs),
                (select_in, select),
            )
        )
    ]
    for load in loads:
        load.start()
    rank = right_basis.shape[1]

    around = [{CORE: other}]
    around += [{X: lax.rem(x + d, nx)} for d in range(1, nx)]
    around += [{Y: lax.rem(y + d, ny)} for d in range(1, ny)]
    around += [{Z: lax.rem(z + d, nz)} for d in range(1, nz)]
    barrier = pltpu.get_barrier_semaphore()
    for device in around:
        pl.semaphore_signal(barrier, inc=1, device_id=device, device_id_type=MESH)

    started = []

    def send(source, target, sems, index, device):
        copy = pltpu.make_async_remote_copy(
            src_ref=source,
            dst_ref=target,
            send_sem=sems.at[0, index],
            recv_sem=sems.at[1, index],
            device_id=device,
            device_id_type=MESH,
        )
        copy.start()
        started.append(copy)
        return copy

    for load in loads:
        load.wait()
    summed_t[...] = momentum[...] + gradient[...].astype(jnp.float32)
    basis_t[...] = right_basis[...].T
    rows = rank // 2
    away = matmul(basis_t[pl.ds(pl.multiple_of(other * rows, rows), rows), :], summed_t[...])
    part_away[...] = away.reshape(part_away.shape)
    pl.semaphore_wait(barrier, len(around))
    order = [lax.rem(x + d, nx) for d in sorted(range(1, nx), key=lambda d: -min(d, nx - d))] + [x]
    core_copies = [
        send(part_away.at[to], core_in.at[to], core_sems, i, {CORE: other})
        for i, to in enumerate(order)
    ]
    home = matmul(basis_t[pl.ds(pl.multiple_of(c * rows, rows), rows), :], summed_t[...])
    part_home[...] = home.reshape(part_home.shape)

    x_copies = []
    for i, to in enumerate(order):
        core_copies[i].wait_recv()
        total = part_home[to] + core_in[to]
        if i < nx - 1:
            chip_sum[to] = total
            x_copies.append(send(chip_sum.at[to], x_in.at[x], x_sems, i, {X: to}))
        else:
            x_in[x] = total
    place = lax.broadcasted_iota(jnp.int32, parity.shape, 0) + z * 2 * half
    shared = jnp.bitwise_and(place, select[...].reshape(1, SKETCH))
    for shift in (8, 4, 2, 1):
        shared = jnp.bitwise_xor(shared, jnp.right_shift(shared, shift))
    parity[...] = (1.0 - 2.0 * jnp.bitwise_and(shared, 1).astype(jnp.float32)).astype(jnp.bfloat16)
    for copy in x_copies:
        copy.wait_recv()
    total = x_in[0]
    for i in range(1, nx):
        total = total + x_in[i]
    own_rows = total.shape[0] // ny
    for i in range(ny):
        part = total[i * own_rows : (i + 1) * own_rows]
        y_out[i] = jnp.concatenate([part[:, :half], part[:, half:]], axis=0)
    y_copies = []
    for d in range(1, ny):
        to = lax.rem(y + d, ny)
        y_copies.append(send(y_out.at[to], y_in.at[y], y_sems, d - 1, {Y: to}))
    y_in[y] = y_out[y]
    for copy in y_copies:
        copy.wait_recv()
    own = y_in[0]
    for i in range(1, ny):
        own = own + y_in[i]

    mine = x * ny + y

    def along_y(buffer, sems):
        copies = []
        for d in range(1, ny):
            block = buffer.at[c, mine]
            copies.append(send(block, block, sems, d - 1, {Y: lax.rem(y + d, ny)}))
        return copies

    def along_x(buffer, sems, waited):
        copies = []
        for i, k in enumerate([0] + [k for d in range(1, ny // 2 + 1) for k in (d, ny - d)][: ny - 1]):
            if k:
                waited[k - 1].wait_recv()
            block = buffer.at[c, x * ny + lax.rem(y - k + ny, ny)]
            for d in range(1, nx):
                device = {X: lax.rem(x + d, nx)}
                copies.append(send(block, block, sems, ny - 1 + i * nx + d, device))
            if k == ny // 2:
                slab = buffer.at[c, pl.ds(x * ny, ny)]
                last = [send(slab, slab, sems, ny - 1 + i * nx, {CORE: other})]
        return copies, last

    def along_core(buffer, sems, waited):
        copies = []
        for d in range(1, nx):
            for copy in waited[d - 1 :: nx - 1]:
                copy.wait_recv()
            slab = buffer.at[c, pl.ds(lax.rem(x - d + nx, nx) * ny, ny)]
            copies.append(send(slab, slab, sems, ny - 1 + ny * nx + d, {CORE: other}))
        return copies

    def unpacked(buffer):
        pieces = []
        for core in range(2):
            for i in range(0, nx * ny, 2):
                a, b = buffer[core, i], buffer[core, i + 1]
                start = core * rows + i * own_rows
                low = jnp.concatenate([a[:own_rows], b[:own_rows]], axis=0)
                high = jnp.concatenate([a[own_rows:], b[own_rows:]], axis=0)
                pieces.append((slice(start, start + 2 * own_rows), low, high))
        return pieces

    left_t[c, mine] = own
    left_y = along_y(left_t, gather_sems.at[0])

    flip = signs[pl.ds(pl.multiple_of(z * 2 * half, 2 * half), 2 * half)]
    flip = flip.reshape(1, 2 * half).astype(jnp.float32)
    low = sign_product(own * flip[:, :half], parity[:half, :])
    high = sign_product(own * flip[:, half:], parity[half:, :])
    term = (low[:own_rows] + high[own_rows:]) * (1.0 / math.sqrt(SKETCH))
    wide = sketch_z.shape[-1]
    sketch_z_out[...] = jnp.concatenate([term[:, :wide], term[:, SKETCH - wide :]], axis=0)
    sketch_copies = [
        send(sketch_z_out, sketch_z.at[z], sketch_sems, d, {Z: lax.rem(z + d, nz)})
        for d in range(1, nz)
    ]
    sketch_z[z] = sketch_z_out[...]

    left_x, left_core = along_x(left_t, gather_sems.at[0], left_y)

    for copy in sketch_copies:
        copy.wait_recv()
    total = sketch_z[0]
    for i in range(1, nz):
        total = total + sketch_z[i]
    sketch_t[c, mine] = total
    sketch_y = along_y(sketch_t, gather_sems.at[1])

    left_core += along_core(left_t, gather_sems.at[0], left_x)
    for copy in left_core:
        copy.wait_recv()

    for top, low, high in unpacked(left_t):
        left_full[top, :half] = low
        left_full[top, half:] = high
    product = matmul_nt(summed_t[...], left_full[...])
    q_out[...] = product.reshape(q_out.shape)
    at = [lax.rem(z + d, nz) for d in range(nz)]
    cut = q_out.shape[1] // 16 * 8 + 8
    upper, lower = pl.ds(0, cut), pl.ds(cut, q_out.shape[1] - cut)
    relayed = [
        send(q_out.at[at[4], upper], q_in.at[5, upper], q_sems, 5, {Z: at[2]}),
        send(q_out.at[at[4], lower], q_in.at[7, lower], q_sems, 7, {Z: at[6]}),
        send(q_out.at[at[3]], q_in.at[4], q_sems, 4, {Z: at[1]}),
        send(q_out.at[at[5]], q_in.at[6], q_sems, 6, {Z: at[7]}),
    ]
    q_copies = [
        send(q_out.at[at[1]], q_in.at[0], q_sems, 0, {Z: at[1]}),
        send(q_out.at[at[7]], q_in.at[1], q_sems, 1, {Z: at[7]}),
    ]

    sketch_x, sketch_core = along_x(sketch_t, gather_sems.at[1], sketch_y)
    for copy in relayed:
        copy.wait_recv()
    q_relay[0] = q_out[at[2]] + q_in[4]
    q_relay[0, upper] += q_in[5, upper]
    q_relay[1] = q_out[at[6]] + q_in[6]
    q_relay[1, lower] += q_in[7, lower]
    q_copies.append(send(q_relay.at[0], q_in.at[2], q_sems, 2, {Z: at[2]}))
    q_copies.append(send(q_relay.at[1], q_in.at[3], q_sems, 3, {Z: at[6]}))
    sketch_core += along_core(sketch_t, gather_sems.at[1], sketch_x)
    for copy in sketch_core:
        copy.wait_recv()

    for top, low, high in unpacked(sketch_t):
        sketch_full[top, :wide] = low
        sketch_full[top, wide:] = high[:, 2 * wide - SKETCH :]
    gram[...] = matmul_nt(sketch_full[...], sketch_full[...])
    gathered = []
    for b in range(rank // BLOCK):
        factor_block(gram, inverse, b)
        if b == 1:
            for copy in q_copies:
                copy.wait_recv()
            q_all[z] = q_out[z] + q_in[0] + q_in[1] + q_in[2] + q_in[3]
            for k, d in enumerate((2, 6, 1, 7)):
                block = q_all.at[z]
                gathered.append(send(block, block, q_sems, nz + k, {Z: at[d]}))

    share = matmul_nt(q_all[z], inverse[...])
    slot = y * 2 + c
    norm_near[slot] = jnp.sum(share * share, axis=0, keepdims=True)
    near = []
    for d in range(1, 2 * ny):
        device = {Y: lax.rem(y + d // 2, ny), CORE: lax.rem(c + d, 2)}
        near.append(send(norm_near.at[slot], norm_near.at[slot], near_sems, d, device))
    left_out[...] = matmul(inverse[...], left_full[...])
    for copy in gathered[:2]:
        copy.wait_recv()
    passed = [
        (q_all.at[at[6], upper], at[2]),
        (q_all.at[at[2], lower], at[6]),
        (q_all.at[at[6]], at[1]),
        (q_all.at[at[2]], at[7]),
    ]
    gathered = gathered[2:] + [
        send(block, block, q_sems, nz + 4 + k, {Z: to}) for k, (block, to) in enumerate(passed)
    ]
    for copy in near:
        copy.wait_recv()
    total = norm_near[0]
    for i in range(1, 2 * ny):
        total = total + norm_near[i]
    slot = z * nx + x
    norm_far[slot] = total
    far = []
    for d in range(1, nz * nx):
        device = {Z: lax.rem(z + d // nx, nz), X: lax.rem(x + d, nx)}
        far.append(send(norm_far.at[slot], norm_far.at[slot], far_sems, d, device))
    for copy in gathered:
        copy.wait_recv()
    right_out[...] = matmul_nt(q_all[...].reshape(right_out.shape), inverse[...])
    for copy in far:
        copy.wait_recv()
    total = norm_far[0]
    for i in range(1, nz * nx):
        total = total + norm_far[i]
    norm_out[...] = jnp.sqrt(total + norm_epsilon)
    for copy in started:
        copy.wait_send()


def split(value):
    high = value.astype(jnp.bfloat16)
    return high, (value - high.astype(jnp.float32)).astype(jnp.bfloat16)


def outputs(
    summed,
    left,
    right,
    norms,
    moved_out,
    basis_out,
    update_out,
    moved,
    basis,
    update,
    sems,
    *,
    steps,
):
    columns, rank = right.shape
    step = columns // steps
    left_high, left_low = split(left[...])
    basis[...] = right[...] / norms[...]
    copies = [pltpu.make_async_copy(basis, basis_out, sems.at[0])]
    copies[0].start()
    for i in range(steps):
        rows = pl.ds(i * step, step)
        both = jnp.concatenate([right[rows, :], basis[rows, :]], axis=0)
        high, low = split(both)
        product = jnp.dot(high, left_low, preferred_element_type=jnp.float32)
        product += jnp.dot(low, left_high, preferred_element_type=jnp.float32)
        product += jnp.dot(high, left_high, preferred_element_type=jnp.float32)
        moved[rows, :] = summed[rows, :] - (1.0 - decay_mu) * product[:step]
        update[rows, :] = (math.sqrt(ROWS * COLS / RANK) * product[step:]).astype(jnp.bfloat16)
        for k, (source, target) in enumerate(((moved, moved_out), (update, update_out))):
            copy = pltpu.make_async_copy(source.at[rows], target.at[rows], sems.at[1 + 2 * i + k])
            copy.start()
            copies.append(copy)
    for copy in copies:
        copy.wait()


def per_device(sizes, momentum, gradient, right_basis, signs, select):
    nz, nx, ny = sizes
    momentum, gradient, right_basis, signs, select = (
        pltpu.with_memory_space_constraint(value, pltpu.HBM)
        for value in (momentum.T, gradient.T, right_basis, signs, select)
    )
    block_cols, block_rows = momentum.shape
    rank = right_basis.shape[1]
    half = block_rows // 2
    own = 2 * rank // (2 * nx * ny)
    wide = 256
    f32 = jnp.float32
    vmem = pl.BlockSpec(memory_space=pltpu.VMEM)
    hbm = pl.BlockSpec(memory_space=pltpu.HBM)
    dma = pltpu.SemaphoreType.DMA
    share = block_cols // nz
    left, right, norms, summed = pl.pallas_call(
        functools.partial(factors, sizes),
        out_shape=(
            jax.ShapeDtypeStruct((rank, block_rows), f32),
            jax.ShapeDtypeStruct((block_cols, rank), f32),
            jax.ShapeDtypeStruct((1, rank), f32),
            jax.ShapeDtypeStruct((block_cols, block_rows), f32),
        ),
        in_specs=[hbm] * 5,
        out_specs=(vmem,) * 4,
        scratch_shapes=[
            pltpu.VMEM((rank, block_cols), f32),
            pltpu.VMEM((block_cols, block_rows), f32),
            pltpu.VMEM((block_cols, block_rows), jnp.bfloat16),
            pltpu.VMEM((block_cols, rank), f32),
            pltpu.VMEM((ROWS,), jnp.int32),
            pltpu.VMEM((SKETCH,), jnp.int32),
            pltpu.VMEM((nx, rank // (2 * nx), block_rows), f32),
            pltpu.VMEM((nx, rank // (2 * nx), block_rows), f32),
            pltpu.VMEM((nx, rank // (2 * nx), block_rows), f32),
            pltpu.VMEM((nx, rank // (2 * nx), block_rows), f32),
            pltpu.VMEM((nx, rank // (2 * nx), block_rows), f32),
            pltpu.VMEM((ny, own, half), f32),
            pltpu.VMEM((ny, own, half), f32),
            pltpu.VMEM((2, nx * ny, own, half), f32),
            pltpu.VMEM((rank, block_rows), f32),
            pltpu.VMEM((block_rows, SKETCH), jnp.bfloat16),
            pltpu.VMEM((own, wide), f32),
            pltpu.VMEM((nz, own, wide), f32),
            pltpu.VMEM((2, nx * ny, own, wide), f32),
            pltpu.VMEM((rank, SKETCH), f32),
            pltpu.VMEM((rank, rank), f32),
            pltpu.VMEM((rank, rank), f32),
            pltpu.VMEM((nz, share, rank), f32),
            pltpu.VMEM((nz, share, rank), f32),
            pltpu.VMEM((2, share, rank), f32),
            pltpu.VMEM((nz, share, rank), f32),
            pltpu.VMEM((2 * ny, 1, rank), f32),
            pltpu.VMEM((nz * nx, 1, rank), f32),
            dma((2, nx)),
            dma((2, nx)),
            dma((2, ny)),
            dma((2, 2, ny + (ny + 1) * nx)),
            dma((2, nz)),
            dma((2, 2 * nz)),
            dma((2, 2 * ny)),
            dma((2, nz * nx)),
            dma((5,)),
        ],
        compiler_params=pltpu.CompilerParams(
            collective_id=0, has_side_effects=True, vmem_limit_bytes=40 << 20
        ),
        name="factors",
    )(
        momentum,
        gradient,
        right_basis,
        signs,
        select,
    )
    steps = 4
    moved, basis, update = pl.pallas_call(
        functools.partial(outputs, steps=steps),
        out_shape=(
            jax.ShapeDtypeStruct((block_cols, block_rows), f32),
            jax.ShapeDtypeStruct((block_cols, rank), f32),
            jax.ShapeDtypeStruct((block_cols, block_rows), jnp.bfloat16),
        ),
        in_specs=[vmem] * 4,
        out_specs=(hbm,) * 3,
        scratch_shapes=[
            pltpu.VMEM((block_cols, block_rows), f32),
            pltpu.VMEM((block_cols, rank), f32),
            pltpu.VMEM((block_cols, block_rows), jnp.bfloat16),
            dma((1 + 2 * steps,)),
        ],
        compiler_params=pltpu.CompilerParams(vmem_limit_bytes=20 << 20),
        name="outputs",
    )(summed, left, right, norms)
    return moved.T, basis, update.T


def solution(mesh):
    devices = mesh.devices
    shape = (mesh.shape["narrow"], 4, 8, 2) if devices.size == 512 else (2, 2, devices.size // 8, 2)
    split = Mesh(devices.reshape(shape), (Z, X, Y, CORE))
    in_specs = (P(Z, WIDE), P(Z, WIDE), P(WIDE, None), P(), P())
    out_specs = (P(Z, WIDE), P(WIDE, None), P(Z, WIDE))
    return jax.shard_map(
        functools.partial(per_device, shape[:3]),
        mesh=split,
        in_specs=in_specs,
        out_specs=out_specs,
        check_vma=False,
    )
```

```python
import functools
import math

import jax
import jax.numpy as jnp
from jax import lax
from jax.experimental import pallas as pl
from jax.experimental.pallas import tpu as pltpu
from jax.sharding import Mesh
from jax.sharding import PartitionSpec as P

ROWS = 4096
COLS = 28672
RANK = 256
SKETCH = 384
Z, X, Y, CORE = "narrow", "wide_0", "wide_1", "wide_2"
WIDE = (X, Y, CORE)
HIGH = lax.Precision.HIGHEST
MESH = pl.DeviceIdType.MESH
BLOCK = 64

decay_mu = 0.95
norm_epsilon = 1e-06


def matmul(a, b):
    return jnp.dot(a, b, precision=HIGH, preferred_element_type=jnp.float32)


def matmul_nt(a, b):
    return lax.dot_general(
        a, b, (((1,), (1,)), ((), ())), precision=HIGH, preferred_element_type=jnp.float32
    )


def matmul_tn(a, b):
    return lax.dot_general(
        a, b, (((0,), (0,)), ((), ())), precision=HIGH, preferred_element_type=jnp.float32
    )


def far_first(size):
    return sorted(range(1, size), key=lambda d: -min(d, size - d))


def sign_product(value, signs):
    rows = value.shape[0]
    pieces = []
    for _ in range(3):
        pieces.append(value.astype(jnp.bfloat16).astype(jnp.float32))
        value = value - pieces[-1]
    stacked = jnp.concatenate(pieces, axis=0).astype(jnp.bfloat16)
    product = jnp.dot(stacked, signs, preferred_element_type=jnp.float32)
    return product[:rows] + product[rows : 2 * rows] + product[2 * rows :]


def factor_block(a_ref, inverse_ref, b):
    n = a_ref.shape[0]
    lo, hi = b * BLOCK, (b + 1) * BLOCK
    tile, off = lo // 128, lo % 128
    lane = lax.broadcasted_iota(jnp.int32, (8, 128), 1)
    sub = lax.broadcasted_iota(jnp.int32, (8, 128), 0)
    groups = BLOCK // 8
    rows = [
        a_ref[lo + 8 * q : lo + 8 * q + 8, tile * 128 : (tile + 1) * 128] for q in range(groups)
    ]
    column = {}

    def spread(panel, first):
        for j in range(8 * panel, 8 * panel + 8):
            for q in range(first, groups):
                column[q, j] = jnp.broadcast_to(rows[q][:, off + j : off + j + 1], (8, 128))

    def row_of(value, k):
        return jnp.broadcast_to(value[k : k + 1, :], (8, 128))

    spread(0, 0)
    for p in range(groups):
        if p + 1 < groups:
            spread(p + 1, p + 1)
        for k in range(8):
            kk = 8 * p + k
            here, below = lane == off + kk, sub > k
            root = lax.rsqrt(row_of(column[p, kk], k))
            pivot = jnp.where(here, root, row_of(rows[p], k) * root)
            scaled = {q: column[q, kk] * root for q in range(p, groups)}
            scaled[p] = jnp.where(below, scaled[p], 0.0)
            for j in range(kk + 1, min(8 * (p + 2), BLOCK)):
                share = row_of(scaled[j // 8], j % 8)
                for q in range(j // 8, groups):
                    column[q, j] = column[q, j] - scaled[q] * share
            for q in range(p + 1, groups):
                rows[q] = jnp.where(here, 0.0, rows[q]) - scaled[q] * pivot
            rest = jnp.where(here & below, 0.0, rows[p]) - scaled[p] * pivot
            rows[p] = jnp.where(sub == k, pivot, rest)
    corner = jnp.concatenate(
        [
            jnp.where((lane >= off) & (lane <= off + 8 * q + sub), row, 0.0)
            for q, row in enumerate(rows)
        ],
        axis=0,
    )
    solved = matmul(corner, a_ref[tile * 128 : (tile + 1) * 128, :])
    cols = lax.broadcasted_iota(jnp.int32, (BLOCK, n), 1)
    placed = jnp.concatenate(
        [corner if t == tile else jnp.zeros_like(corner) for t in range(n // 128)], axis=1
    )
    solved = jnp.where((cols >= lo) & (cols < hi), placed, solved)
    inverse_ref[lo:hi, :] = jnp.where(cols < hi, solved, 0.0)
    if hi < n:
        start = hi // 128 * 128
        outer = matmul_tn(solved[:, start:], solved)
        cols = lax.broadcasted_iota(jnp.int32, (n - hi, n), 1)
        kept = jnp.where((cols >= lo) & (cols < hi), 0.0, a_ref[hi:n, :])
        a_ref[hi:n, :] = kept - outer[hi - start :, :]


def factors(
    sizes,
    momentum_in,
    gradient_in,
    basis_in,
    signs_in,
    select_in,
    left_out,
    right_out,
    norm_out,
    summed_t,
    basis_t,
    momentum,
    gradient,
    right_basis,
    signs,
    select,
    part_away,
    part_home,
    core_in,
    chip_sum,
    x_in,
    y_out,
    y_in,
    left_t,
    left_full,
    parity,
    sketch_z_out,
    sketch_z,
    sketch_t,
    sketch_full,
    gram,
    inverse,
    q_out,
    q_in,
    q_relay,
    q_all,
    norm_near,
    norm_far,
    core_sems,
    x_sems,
    y_sems,
    gather_sems,
    sketch_sems,
    q_sems,
    near_sems,
    far_sems,
    load_sems,
):
    nz, nx, ny = sizes
    z, x, y, c = (lax.axis_index(name) for name in (Z, X, Y, CORE))
    other = 1 - c
    half = summed_t.shape[1] // 2
    loads = [
        pltpu.make_async_copy(source, target, load_sems.at[i])
        for i, (source, target) in enumerate(
            (
                (momentum_in, momentum),
                (gradient_in, gradient),
                (basis_in, right_basis),
                (signs_in, signs),
                (select_in, select),
            )
        )
    ]
    for load in loads:
        load.start()
    rank = right_basis.shape[1]

    around = [{CORE: other}]
    around += [{X: lax.rem(x + d, nx)} for d in range(1, nx)]
    around += [{Y: lax.rem(y + d, ny)} for d in range(1, ny)]
    around += [{Z: lax.rem(z + d, nz)} for d in range(1, nz)]
    barrier = pltpu.get_barrier_semaphore()
    for device in around:
        pl.semaphore_signal(barrier, inc=1, device_id=device, device_id_type=MESH)

    started = []

    def send(source, target, sems, index, device):
        copy = pltpu.make_async_remote_copy(
            src_ref=source,
            dst_ref=target,
            send_sem=sems.at[0, index],
            recv_sem=sems.at[1, index],
            device_id=device,
            device_id_type=MESH,
        )
        copy.start()
        started.append(copy)
        return copy

    for load in loads:
        load.wait()
    summed_t[...] = momentum[...] + gradient[...].astype(jnp.float32)
    basis_t[...] = right_basis[...].T
    rows = rank // 2
    away = matmul(basis_t[pl.ds(pl.multiple_of(other * rows, rows), rows), :], summed_t[...])
    part_away[...] = away.reshape(part_away.shape)
    pl.semaphore_wait(barrier, len(around))
    order = [lax.rem(x + d, nx) for d in far_first(nx)] + [x]
    core_copies = [
        send(part_away.at[to], core_in.at[to], core_sems, i, {CORE: other})
        for i, to in enumerate(order)
    ]
    home = matmul(basis_t[pl.ds(pl.multiple_of(c * rows, rows), rows), :], summed_t[...])
    part_home[...] = home.reshape(part_home.shape)

    x_copies = []
    for i, to in enumerate(order):
        core_copies[i].wait_recv()
        total = part_home[to] + core_in[to]
        if i < nx - 1:
            chip_sum[to] = total
            x_copies.append(send(chip_sum.at[to], x_in.at[x], x_sems, i, {X: to}))
        else:
            x_in[x] = total
    place = lax.broadcasted_iota(jnp.int32, parity.shape, 0) + z * 2 * half
    shared = jnp.bitwise_and(place, select[...].reshape(1, SKETCH))
    for shift in (8, 4, 2, 1):
        shared = jnp.bitwise_xor(shared, jnp.right_shift(shared, shift))
    parity[...] = (1.0 - 2.0 * jnp.bitwise_and(shared, 1).astype(jnp.float32)).astype(jnp.bfloat16)
    for copy in x_copies:
        copy.wait_recv()
    total = x_in[0]
    for i in range(1, nx):
        total = total + x_in[i]
    own_rows = total.shape[0] // ny
    for i in range(ny):
        part = total[i * own_rows : (i + 1) * own_rows]
        y_out[i] = jnp.concatenate([part[:, :half], part[:, half:]], axis=0)
    y_copies = []
    for d in far_first(ny):
        to = lax.rem(y + d, ny)
        y_copies.append(send(y_out.at[to], y_in.at[y], y_sems, d - 1, {Y: to}))
    y_in[y] = y_out[y]
    for copy in y_copies:
        copy.wait_recv()
    own = y_in[0]
    for i in range(1, ny):
        own = own + y_in[i]

    mine = x * ny + y

    def along_y(buffer, sems):
        copies = {}
        for d in far_first(ny):
            block = buffer.at[c, mine]
            copies[d] = send(block, block, sems, d - 1, {Y: lax.rem(y + d, ny)})
        return copies

    def along_x(buffer, sems, waited):
        copies = {d: [] for d in range(1, nx)}
        for i, k in enumerate([0] + [k for d in range(1, ny // 2 + 1) for k in (d, ny - d)][: ny - 1]):
            if k:
                waited[k].wait_recv()
            block = buffer.at[c, x * ny + lax.rem(y - k + ny, ny)]
            for d in far_first(nx):
                device = {X: lax.rem(x + d, nx)}
                copies[d].append(send(block, block, sems, ny - 1 + i * nx + d, device))
            if k == ny // 2:
                slab = buffer.at[c, pl.ds(x * ny, ny)]
                last = [send(slab, slab, sems, ny - 1 + i * nx, {CORE: other})]
        return copies, last

    def along_core(buffer, sems, waited):
        copies = []
        for d in reversed(far_first(nx)):
            for copy in waited[d]:
                copy.wait_recv()
            slab = buffer.at[c, pl.ds(lax.rem(x - d + nx, nx) * ny, ny)]
            copies.append(send(slab, slab, sems, ny - 1 + ny * nx + d, {CORE: other}))
        return copies

    def unpacked(buffer):
        pieces = []
        for core in range(2):
            for i in range(0, nx * ny, 2):
                a, b = buffer[core, i], buffer[core, i + 1]
                start = core * rows + i * own_rows
                low = jnp.concatenate([a[:own_rows], b[:own_rows]], axis=0)
                high = jnp.concatenate([a[own_rows:], b[own_rows:]], axis=0)
                pieces.append((slice(start, start + 2 * own_rows), low, high))
        return pieces

    left_t[c, mine] = own
    left_y = along_y(left_t, gather_sems.at[0])

    flip = signs[pl.ds(pl.multiple_of(z * 2 * half, 2 * half), 2 * half)]
    flip = flip.reshape(1, 2 * half).astype(jnp.float32)
    low = sign_product(own * flip[:, :half], parity[:half, :])
    high = sign_product(own * flip[:, half:], parity[half:, :])
    term = (low[:own_rows] + high[own_rows:]) * (1.0 / math.sqrt(SKETCH))
    wide = sketch_z.shape[-1]
    sketch_z_out[...] = jnp.concatenate([term[:, :wide], term[:, SKETCH - wide :]], axis=0)
    sketch_copies = [
        send(sketch_z_out, sketch_z.at[z], sketch_sems, d, {Z: lax.rem(z + d, nz)})
        for d in far_first(nz)
    ]
    sketch_z[z] = sketch_z_out[...]

    left_x, left_core = along_x(left_t, gather_sems.at[0], left_y)

    for copy in sketch_copies:
        copy.wait_recv()
    total = sketch_z[0]
    for i in range(1, nz):
        total = total + sketch_z[i]
    sketch_t[c, mine] = total
    sketch_y = along_y(sketch_t, gather_sems.at[1])

    left_core += along_core(left_t, gather_sems.at[0], left_x)
    for copy in left_core:
        copy.wait_recv()

    for top, low, high in unpacked(left_t):
        left_full[top, :half] = low
        left_full[top, half:] = high
    product = matmul_nt(summed_t[...], left_full[...])
    q_out[...] = product.reshape(q_out.shape)
    at = [lax.rem(z + d, nz) for d in range(nz)]
    cut = q_out.shape[1] // 16 * 8 + 8
    upper, lower = pl.ds(0, cut), pl.ds(cut, q_out.shape[1] - cut)
    relayed = [
        send(q_out.at[at[4], upper], q_in.at[5, upper], q_sems, 5, {Z: at[2]}),
        send(q_out.at[at[4], lower], q_in.at[7, lower], q_sems, 7, {Z: at[6]}),
        send(q_out.at[at[3]], q_in.at[4], q_sems, 4, {Z: at[1]}),
        send(q_out.at[at[5]], q_in.at[6], q_sems, 6, {Z: at[7]}),
    ]
    q_copies = [
        send(q_out.at[at[1]], q_in.at[0], q_sems, 0, {Z: at[1]}),
        send(q_out.at[at[7]], q_in.at[1], q_sems, 1, {Z: at[7]}),
    ]

    sketch_x, sketch_core = along_x(sketch_t, gather_sems.at[1], sketch_y)
    sketch_core += along_core(sketch_t, gather_sems.at[1], sketch_x)
    for copy in relayed:
        copy.wait_recv()
    q_relay[0] = q_out[at[2]] + q_in[4]
    q_relay[0, upper] += q_in[5, upper]
    q_relay[1] = q_out[at[6]] + q_in[6]
    q_relay[1, lower] += q_in[7, lower]
    q_copies.append(send(q_relay.at[0], q_in.at[2], q_sems, 2, {Z: at[2]}))
    q_copies.append(send(q_relay.at[1], q_in.at[3], q_sems, 3, {Z: at[6]}))
    for copy in sketch_core:
        copy.wait_recv()

    for top, low, high in unpacked(sketch_t):
        sketch_full[top, :wide] = low
        sketch_full[top, wide:] = high[:, 2 * wide - SKETCH :]
    gram[...] = matmul_nt(sketch_full[...], sketch_full[...])
    gathered = []
    for b in range(rank // BLOCK):
        factor_block(gram, inverse, b)
        if b == 1:
            for copy in q_copies:
                copy.wait_recv()
            q_all[z] = q_out[z] + q_in[0] + q_in[1] + q_in[2] + q_in[3]
            for k, d in enumerate((2, 6, 1, 7)):
                block = q_all.at[z]
                gathered.append(send(block, block, q_sems, nz + k, {Z: at[d]}))

    share = matmul_nt(q_all[z], inverse[...])
    slot = y * 2 + c
    norm_near[slot] = jnp.sum(share * share, axis=0, keepdims=True)
    near = []
    for d in sorted(range(1, 2 * ny), key=lambda d: -min(d // 2, ny - d // 2)):
        device = {Y: lax.rem(y + d // 2, ny), CORE: lax.rem(c + d, 2)}
        near.append(send(norm_near.at[slot], norm_near.at[slot], near_sems, d, device))
    left_out[...] = matmul(inverse[...], left_full[...])
    for copy in gathered[:2]:
        copy.wait_recv()
    passed = [
        (q_all.at[at[6], upper], at[2]),
        (q_all.at[at[2], lower], at[6]),
        (q_all.at[at[6]], at[1]),
        (q_all.at[at[2]], at[7]),
    ]
    gathered = gathered[2:] + [
        send(block, block, q_sems, nz + 4 + k, {Z: to}) for k, (block, to) in enumerate(passed)
    ]
    for copy in near:
        copy.wait_recv()
    total = norm_near[0]
    for i in range(1, 2 * ny):
        total = total + norm_near[i]
    slot = z * nx + x
    norm_far[slot] = total
    far = []
    for d in sorted(
        range(1, nz * nx),
        key=lambda d: -min(d // nx, nz - d // nx) - min(d % nx, nx - d % nx),
    ):
        device = {Z: lax.rem(z + d // nx, nz), X: lax.rem(x + d, nx)}
        far.append(send(norm_far.at[slot], norm_far.at[slot], far_sems, d, device))
    for copy in gathered:
        copy.wait_recv()
    right_out[...] = matmul_nt(q_all[...].reshape(right_out.shape), inverse[...])
    for copy in far:
        copy.wait_recv()
    total = norm_far[0]
    for i in range(1, nz * nx):
        total = total + norm_far[i]
    norm_out[...] = jnp.sqrt(total + norm_epsilon)
    for copy in started:
        copy.wait_send()


def split(value):
    high = value.astype(jnp.bfloat16)
    return high, (value - high.astype(jnp.float32)).astype(jnp.bfloat16)


def outputs(
    summed,
    left,
    right,
    norms,
    moved_out,
    basis_out,
    update_out,
    moved,
    basis,
    update,
    sems,
    *,
    steps,
):
    columns, rank = right.shape
    step = columns // steps
    left_high, left_low = split(left[...])
    basis[...] = right[...] / norms[...]
    copies = [pltpu.make_async_copy(basis, basis_out, sems.at[0])]
    copies[0].start()
    for i in range(steps):
        rows = pl.ds(i * step, step)
        both = jnp.concatenate([right[rows, :], basis[rows, :]], axis=0)
        high, low = split(both)
        product = jnp.dot(high, left_low, preferred_element_type=jnp.float32)
        product += jnp.dot(low, left_high, preferred_element_type=jnp.float32)
        product += jnp.dot(high, left_high, preferred_element_type=jnp.float32)
        moved[rows, :] = summed[rows, :] - (1.0 - decay_mu) * product[:step]
        update[rows, :] = (math.sqrt(ROWS * COLS / RANK) * product[step:]).astype(jnp.bfloat16)
        for k, (source, target) in enumerate(((moved, moved_out), (update, update_out))):
            copy = pltpu.make_async_copy(source.at[rows], target.at[rows], sems.at[1 + 2 * i + k])
            copy.start()
            copies.append(copy)
    for copy in copies:
        copy.wait()


def per_device(sizes, momentum, gradient, right_basis, signs, select):
    nz, nx, ny = sizes
    momentum, gradient, right_basis, signs, select = (
        pltpu.with_memory_space_constraint(value, pltpu.HBM)
        for value in (momentum.T, gradient.T, right_basis, signs, select)
    )
    block_cols, block_rows = momentum.shape
    rank = right_basis.shape[1]
    half = block_rows // 2
    own = 2 * rank // (2 * nx * ny)
    wide = 256
    f32 = jnp.float32
    vmem = pl.BlockSpec(memory_space=pltpu.VMEM)
    hbm = pl.BlockSpec(memory_space=pltpu.HBM)
    dma = pltpu.SemaphoreType.DMA
    share = block_cols // nz
    left, right, norms, summed = pl.pallas_call(
        functools.partial(factors, sizes),
        out_shape=(
            jax.ShapeDtypeStruct((rank, block_rows), f32),
            jax.ShapeDtypeStruct((block_cols, rank), f32),
            jax.ShapeDtypeStruct((1, rank), f32),
            jax.ShapeDtypeStruct((block_cols, block_rows), f32),
        ),
        in_specs=[hbm] * 5,
        out_specs=(vmem,) * 4,
        scratch_shapes=[
            pltpu.VMEM((rank, block_cols), f32),
            pltpu.VMEM((block_cols, block_rows), f32),
            pltpu.VMEM((block_cols, block_rows), jnp.bfloat16),
            pltpu.VMEM((block_cols, rank), f32),
            pltpu.VMEM((ROWS,), jnp.int32),
            pltpu.VMEM((SKETCH,), jnp.int32),
            pltpu.VMEM((nx, rank // (2 * nx), block_rows), f32),
            pltpu.VMEM((nx, rank // (2 * nx), block_rows), f32),
            pltpu.VMEM((nx, rank // (2 * nx), block_rows), f32),
            pltpu.VMEM((nx, rank // (2 * nx), block_rows), f32),
            pltpu.VMEM((nx, rank // (2 * nx), block_rows), f32),
            pltpu.VMEM((ny, own, half), f32),
            pltpu.VMEM((ny, own, half), f32),
            pltpu.VMEM((2, nx * ny, own, half), f32),
            pltpu.VMEM((rank, block_rows), f32),
            pltpu.VMEM((block_rows, SKETCH), jnp.bfloat16),
            pltpu.VMEM((own, wide), f32),
            pltpu.VMEM((nz, own, wide), f32),
            pltpu.VMEM((2, nx * ny, own, wide), f32),
            pltpu.VMEM((rank, SKETCH), f32),
            pltpu.VMEM((rank, rank), f32),
            pltpu.VMEM((rank, rank), f32),
            pltpu.VMEM((nz, share, rank), f32),
            pltpu.VMEM((nz, share, rank), f32),
            pltpu.VMEM((2, share, rank), f32),
            pltpu.VMEM((nz, share, rank), f32),
            pltpu.VMEM((2 * ny, 1, rank), f32),
            pltpu.VMEM((nz * nx, 1, rank), f32),
            dma((2, nx)),
            dma((2, nx)),
            dma((2, ny)),
            dma((2, 2, ny + (ny + 1) * nx)),
            dma((2, nz)),
            dma((2, 2 * nz)),
            dma((2, 2 * ny)),
            dma((2, nz * nx)),
            dma((5,)),
        ],
        compiler_params=pltpu.CompilerParams(
            collective_id=0, has_side_effects=True, vmem_limit_bytes=40 << 20
        ),
        name="factors",
    )(
        momentum,
        gradient,
        right_basis,
        signs,
        select,
    )
    steps = 4
    moved, basis, update = pl.pallas_call(
        functools.partial(outputs, steps=steps),
        out_shape=(
            jax.ShapeDtypeStruct((block_cols, block_rows), f32),
            jax.ShapeDtypeStruct((block_cols, rank), f32),
            jax.ShapeDtypeStruct((block_cols, block_rows), jnp.bfloat16),
        ),
        in_specs=[vmem] * 4,
        out_specs=(hbm,) * 3,
        scratch_shapes=[
            pltpu.VMEM((block_cols, block_rows), f32),
            pltpu.VMEM((block_cols, rank), f32),
            pltpu.VMEM((block_cols, block_rows), jnp.bfloat16),
            dma((1 + 2 * steps,)),
        ],
        compiler_params=pltpu.CompilerParams(vmem_limit_bytes=20 << 20),
        name="outputs",
    )(summed, left, right, norms)
    return moved.T, basis, update.T


def solution(mesh):
    devices = mesh.devices
    shape = (mesh.shape["narrow"], 4, 8, 2) if devices.size == 512 else (2, 2, devices.size // 8, 2)
    split = Mesh(devices.reshape(shape), (Z, X, Y, CORE))
    in_specs = (P(Z, WIDE), P(Z, WIDE), P(WIDE, None), P(), P())
    out_specs = (P(Z, WIDE), P(WIDE, None), P(Z, WIDE))
    return jax.shard_map(
        functools.partial(per_device, shape[:3]),
        mesh=split,
        in_specs=in_specs,
        out_specs=out_specs,
        check_vma=False,
    )
```
